256 devices in a mesh: dp: 64 (over y, z_hi, x), mp: 4 (over z_lo, core).
Axes of the slice: x: 4, y: 4, z: 8 (z_hi: 4, z_lo: 2; z = z_hi * 2 + z_lo), core: 2. Of those that a mesh axis runs over, the one named last changes fastest.
Arguments:
- layer_inputs: bfloat16 [2, 24576, 1024], P(None, 'dp'), may hold values from -11 to 11, as said below
- out_grads: bfloat16 [2, 24576, 1024], P(None, 'dp'), may hold values from -11 to 11, as said below
- damping: float32 [4], replicated, may hold values from 0.1 to 0.5
- owners: int32 [4], replicated, may hold values from 0 to 64, as said below
- old_inverse: bfloat16 [4, 1024, 1024], P('mp'), may hold values from -1.5 to 1.5, as said below
- step_size: float32 [2], replicated, may hold values from 100 to 400
Outputs:
- updates: bfloat16 [2, 1024, 1024], P(None, 'dp')
The draws below stay inside these ranges and needn't reach their ends.
Inputs may be any that keep to these rules, and one draw needn't show every extreme that they name: `layer_inputs`: layer inputs: rows of mixed scale. `out_grads`: output gradients: rows of mixed scale. `old_inverse`: each kept inverse is symmetric. `owners`: exactly one factor has the value 64.
All inputs are finite; a program needn't handle non-finite values.
Results may differ from the reference program's by a relative error of at most 0.012.
Values may be sent and summed in bfloat16 or wider, within the bound.
No kernel may reach another device: no remote copies, remote signals or barrier semaphores. Data moves between devices by JAX's collectives and lax.ppermute only.
A program may use at most 128 MiB of HBM per device.

```python
import math
import jax
import jax.numpy as jnp
from jax import lax

D = 1024
LAYERS = 2
FACTORS = 4
TOKENS = 24576
N_DP = 64


def rough_rows(key):
    first, second = jax.random.split(key, 2)
    base = jnp.clip(jax.random.normal(first, (LAYERS, TOKENS, D), jnp.float32), -5.0, 5.0)
    ramp = 0.5 + jnp.arange(TOKENS, dtype=jnp.float32) / TOKENS
    rough = jax.random.uniform(second, (LAYERS, TOKENS, 1), jnp.float32, 0.7, 1.4)
    return jnp.clip(base * ramp[None, :, None] * rough, -10.5, 10.5)


def draw_layer_inputs(key, part):
    return rough_rows(jax.random.fold_in(key, 11)).astype(jnp.bfloat16)


def draw_out_grads(key, part):
    return rough_rows(jax.random.fold_in(key, 23)).astype(jnp.bfloat16)


def draw_owners(key, part):
    first, second = jax.random.split(jax.random.fold_in(key, 51), 2)
    chosen = jax.random.randint(first, (FACTORS,), 0, N_DP)
    kept_slot = jax.random.randint(second, (), 0, FACTORS)
    zero_slot = (kept_slot + 1) % FACTORS
    slots = jnp.arange(FACTORS, dtype=jnp.int32)
    chosen = jnp.where(slots == zero_slot, 0, chosen)
    return jnp.where(slots == kept_slot, N_DP, chosen).astype(jnp.int32)


def draw_old_inverse(key, part):
    first, second = jax.random.split(jax.random.fold_in(key, 37))
    noise = jax.random.normal(first, (FACTORS, D, D), jnp.float32) * (0.4 / D ** 0.5)
    noise = jnp.clip(noise, -0.5, 0.5)
    symmetric = 0.5 * (noise + jnp.swapaxes(noise, 1, 2))
    diagonal = jnp.exp(jax.random.uniform(second, (FACTORS, D), jnp.float32, jnp.log(0.5), jnp.log(1.0)))
    identity = jnp.eye(D, dtype=jnp.float32)
    return (symmetric + diagonal[:, :, None] * identity[None]).astype(jnp.bfloat16)


def setup_inputs(seed: int = 0) -> dict:
    seeds = jax.random.split(jax.random.key(seed), 7)
    layer_inputs = draw_layer_inputs(jax.random.fold_in(seeds[6], 71), 0)
    out_grads = draw_out_grads(jax.random.fold_in(seeds[6], 71), 0)
    damping = jnp.clip(jnp.exp(jax.random.uniform(seeds[2], (FACTORS,), jnp.float32, math.log(0.1), math.log(0.5))), 0.1, 0.5)
    owners = draw_owners(jax.random.fold_in(seeds[6], 71), 0)
    old_inverse = draw_old_inverse(jax.random.fold_in(seeds[6], 71), 0)
    step_size = jnp.clip(jnp.exp(jax.random.uniform(seeds[5], (LAYERS,), jnp.float32, math.log(100.0), math.log(400.0))), 100.0, 400.0)
    return dict(layer_inputs=layer_inputs, out_grads=out_grads, damping=damping, owners=owners, old_inverse=old_inverse, step_size=step_size)


def invert_damped(factor, shift):
    identity = jnp.eye(factor.shape[0], dtype=factor.dtype)
    lower = jnp.linalg.cholesky(factor + shift * identity)
    return jax.scipy.linalg.cho_solve((lower, True), identity).astype(jnp.bfloat16)

def reference(layer_inputs, out_grads, damping, owners, old_inverse, step_size):
    count_all = layer_inputs.shape[1]
    highest = lax.Precision.HIGHEST
    inverses = []
    for layer in range(LAYERS):
        inputs_wide = layer_inputs[layer].astype(jnp.float32)
        grads_wide = out_grads[layer].astype(jnp.float32)
        for which, source_rows in ((0, inputs_wide), (1, grads_wide)):
            factor_id = 2 * layer + which
            factor = jnp.dot(source_rows.T, source_rows, precision=highest) / count_all
            computed = invert_damped(factor, damping[factor_id])
            inverses.append(jnp.where(owners[factor_id] < N_DP, computed, old_inverse[factor_id]))
    results = []
    for layer in range(LAYERS):
        inputs_wide = layer_inputs[layer].astype(jnp.float32)
        grads_wide = out_grads[layer].astype(jnp.float32)
        gradient = jnp.dot(grads_wide.T, inputs_wide, precision=highest) / count_all
        gradient_low = gradient.astype(jnp.bfloat16)
        half = jnp.dot(gradient_low.astype(jnp.float32), inverses[2 * layer].astype(jnp.float32), precision=highest).astype(jnp.bfloat16)
        product = jnp.dot(inverses[2 * layer + 1].astype(jnp.float32), half.astype(jnp.float32), precision=highest)
        results.append((step_size[layer] * product).astype(jnp.bfloat16))
    return jnp.stack(results)
```

```python
import functools

import jax
import jax.numpy as jnp
import numpy as np
from jax import lax
from jax.experimental import pallas as pl
from jax.experimental.pallas import tpu as pltpu
from jax.sharding import Mesh
from jax.sharding import PartitionSpec as P


RING = 4
TILE = 128
HIGHEST = lax.Precision.HIGHEST
VMEM = pl.BlockSpec(memory_space=pltpu.VMEM)
SMEM = pl.BlockSpec(memory_space=pltpu.SMEM)
AT_X, AT_Y, AT_Z, AT_LAYER, AT_SIDE, AT_ROW, AT_FRESH = range(7)


def params(mib):
    return pltpu.CompilerParams(vmem_limit_bytes=mib << 20)


def call(kernel, name, out_shape, in_specs, scratch=(), flops=0, aliases=None, mib=4):
    return pl.pallas_call(
        kernel,
        out_shape=out_shape,
        in_specs=in_specs,
        out_specs=jax.tree.map(lambda _: VMEM, out_shape),
        scratch_shapes=scratch,
        compiler_params=params(mib),
        cost_estimate=pl.CostEstimate(flops=flops, transcendentals=0, bytes_accessed=0),
        input_output_aliases=aliases or {},
        name=name,
    )


def upper(tiles):
    return [(i, j) for i in range(tiles) for j in range(i, tiles)]


def plus(coordinate, shift):
    return lax.rem(coordinate + shift + RING, RING)


def stats_kernel(where, inputs, grads, *refs):
    outs, (source, factor, slab) = refs[:-3], refs[-3:]
    width = inputs.shape[1]
    tiles = width // TILE
    side = where[AT_SIDE]

    @pl.when(side == 0)
    def _():
        source[...] = inputs[...]

    @pl.when(side != 0)
    def _():
        source[...] = grads[...]

    contract = (((0,), (0,)), ((), ()))
    n = 0
    for i in range(tiles):
        rows = lax.dot_general(
            source[:, i * TILE : (i + 1) * TILE],
            source[:, i * TILE :],
            contract,
            preferred_element_type=jnp.float32,
        )
        for j in range(tiles - i):
            factor[n] = rows[:, j * TILE : (j + 1) * TILE]
            n += 1
    half = width // 2
    mine = grads[:, pl.ds(pl.multiple_of(side * half, half), half)]
    for i in range(tiles // 2):
        rows = lax.dot_general(
            mine[:, i * TILE : (i + 1) * TILE],
            inputs[...],
            contract,
            preferred_element_type=jnp.float32,
        )
        for j in range(tiles):
            slab[i * tiles + j] = rows[:, j * TILE : (j + 1) * TILE]
    first = 0
    for group, (store, at) in enumerate(
        ((factor, AT_X), (factor, AT_Y), (slab, AT_X), (slab, AT_Y))
    ):
        if group == 2:
            first = 0
        count = outs[group * RING].shape[0] // TILE
        for shift in range(RING):
            out = outs[group * RING + shift]
            chunk = plus(where[at], shift)
            for b in range(count):
                out[b * TILE : (b + 1) * TILE, :] = store[first + chunk * count + b]
        first += count * RING


def local_stats(where, inputs, grads, counts):
    _, tokens, width = inputs.shape
    tiles = width // TILE
    outs = [
        jax.ShapeDtypeStruct((c * TILE, TILE), jnp.float32) for c in counts for _ in range(RING)
    ]
    pick = pl.BlockSpec((None, tokens, width), lambda i, where: (where[AT_LAYER], 0, 0))
    return pl.pallas_call(
        stats_kernel,
        out_shape=outs,
        grid_spec=pltpu.PrefetchScalarGridSpec(
            num_scalar_prefetch=1,
            grid=(1,),
            in_specs=[pick, pick],
            out_specs=[pl.BlockSpec(o.shape, lambda i, where: (0, 0)) for o in outs],
            scratch_shapes=[
                pltpu.VMEM((tokens, width), inputs.dtype),
                pltpu.VMEM((len(upper(tiles)), TILE, TILE), jnp.float32),
                pltpu.VMEM((tiles * tiles // 2, TILE, TILE), jnp.float32),
            ],
        ),
        compiler_params=params(24),
        name="local_stats",
    )(where, inputs, grads)


def split_kernel(ats, where, *refs):
    for h, at in enumerate(ats):
        ins = refs[h * RING : (h + 1) * RING]
        outs = refs[(len(ats) + h) * RING : (len(ats) + h + 1) * RING]
        rows = outs[0].shape[0]
        for shift in range(RING):
            part = pl.ds(pl.multiple_of(plus(where[at], shift) * rows, 8), rows)
            a, b, c, d = (ref[part, :] for ref in ins)
            outs[shift][...] = (a + b) + (c + d)


def split_sum(where, halves, ats, name):
    flat = [a for half in halves for a in half]
    outs = [jax.ShapeDtypeStruct((a.shape[0] // RING, TILE), a.dtype) for a in flat]
    got = call(
        functools.partial(split_kernel, ats), name, outs, [SMEM] + [VMEM] * len(flat)
    )(where, *flat)
    return got[:RING], got[RING:]


def total_kernel(scale, *refs):
    outs = refs[-2:]
    for h, out in enumerate(outs):
        a, b, c, d = (ref[...] for ref in refs[h * RING : (h + 1) * RING])
        out[...] = (((a + b) + (c + d)) * scale).astype(out.dtype)


def total(halves, scale, dtype, name):
    flat = [a for half in halves for a in half]
    outs = [jax.ShapeDtypeStruct(half[0].shape, dtype) for half in halves]
    return call(functools.partial(total_kernel, scale), name, outs, [VMEM] * len(flat))(*flat)


def place_kernel(ats, where, *refs):
    for h, at in enumerate(ats):
        out = refs[len(ats) * RING + h]
        for shift in range(RING):
            piece = refs[h * RING + shift]
            rows = piece.shape[0]
            to = pl.multiple_of(plus(where[at], -shift) * rows, 16)
            out[pl.ds(to, rows), :] = piece[...]


def place(where, halves, ats, name):
    flat = [a for half in halves for a in half]
    outs = [
        jax.ShapeDtypeStruct((half[0].shape[0] * RING, TILE), half[0].dtype) for half in halves
    ]
    return call(
        functools.partial(place_kernel, ats), name, outs, [SMEM] + [VMEM] * len(flat)
    )(where, *flat)


def send(a, axis, shift):
    return lax.ppermute(a, axis, [(i, (i + shift) % RING) for i in range(RING)])


def swap(half, axis):
    return [half[0]] + [send(half[s], axis, s) for s in range(1, RING)]


def spread(a, axis):
    return [a] + [send(a, axis, s) for s in range(1, RING)]


def row_of(x, t):
    return jnp.broadcast_to(x[t : t + 1, :], x.shape)


def column_of(x, t):
    return jnp.broadcast_to(x[:, t : t + 1], x.shape)


def invert_tile(tile):
    lane = lax.broadcasted_iota(jnp.int32, (8, TILE), 1)
    sub = lax.broadcasted_iota(jnp.int32, (8, TILE), 0)
    for start in range(0, TILE, 8):
        inside = (lane >= start) & (lane < start + 8)
        rows = tile[start : start + 8, :]
        columns = [column_of(rows, start + t) for t in range(8)]
        strip = jnp.where(inside, (lane - start == sub).astype(jnp.float32), rows)
        for t in range(8):
            here = sub == t
            pivot = 1.0 / row_of(columns[t], t)
            for j in range(t + 1, 8):
                r = row_of(columns[j], t) * pivot
                columns[j] = jnp.where(here, r, columns[j] - columns[t] * r)
            r = row_of(strip, t) * pivot
            strip = jnp.where(here, r, strip - columns[t] * r)
        pivots = [row_of(strip, t) for t in range(8)]
        for other in range(0, TILE, 8):
            if other != start:
                block = tile[other : other + 8, :]
                left = jnp.where(inside, 0.0, block)
                for t in range(8):
                    left = left - column_of(block, start + t) * pivots[t]
                tile[other : other + 8, :] = left
        tile[start : start + 8, :] = strip


def dot(a, b):
    return jnp.dot(a, b, preferred_element_type=jnp.float32, precision=HIGHEST)


def eliminate(ks, w, y, tile):
    tiles = w.shape[0] // TILE

    def step(k, carry):
        here = pl.ds(pl.multiple_of(k * TILE, TILE), TILE)
        tile[...] = w[here, here]
        invert_tile(tile)
        w[here, here] = tile[...]
        for kk in ks:
            if kk < tiles - 1:

                @pl.when(k == kk)
                def _():
                    start, lo = kk * TILE, (kk + 1) * TILE
                    panel = w[start:lo, lo:]
                    scaled = dot(tile[...], panel)
                    w[start:lo, lo:] = scaled
                    y[:, lo:] -= dot(y[:, start:lo], scaled)
                    turned = panel.T
                    for i in range(kk + 1, tiles):
                        o = (i - kk - 1) * TILE
                        w[i * TILE : (i + 1) * TILE, i * TILE :] -= dot(
                            turned[o : o + TILE, :], scaled[:, o:]
                        )

        return carry

    lax.fori_loop(ks[0], ks[-1] + 1, step, 0)


def substitute_back(w, y, x):
    tiles = w.shape[0] // TILE
    for k in range(tiles):
        c = slice(k * TILE, (k + 1) * TILE)
        x[:, c] = dot(y[:, c], w[c, c])
    for k in reversed(range(tiles - 1)):
        c, lo = slice(k * TILE, (k + 1) * TILE), (k + 1) * TILE
        x[:, c] -= lax.dot_general(
            x[:, lo:],
            w[c, lo:],
            (((1,), (1,)), ((), ())),
            preferred_element_type=jnp.float32,
            precision=HIGHEST,
        )


def first_kernel(ks, where, shift, table, *refs):
    pieces, (w, y, tile) = refs[: 2 * RING], refs[2 * RING :]
    line = lax.broadcasted_iota(jnp.int32, (TILE, TILE), 0)
    damp = jnp.where(line == lax.broadcasted_iota(jnp.int32, (TILE, TILE), 1), shift[0], 0.0)
    base = 0
    for h, at in enumerate((AT_X, AT_Y)):
        count = pieces[h * RING].shape[0] // TILE
        for s in range(RING):
            for b in range(count):
                n = base + plus(where[at], -s) * count + b
                i, j = table[0, n], table[1, n]
                block = pieces[h * RING + s][b * TILE : (b + 1) * TILE, :]
                block = block + jnp.where(i == j, 1.0, 0.0) * damp
                rows = pl.ds(pl.multiple_of(i * TILE, TILE), TILE)
                w[rows, pl.ds(pl.multiple_of(j * TILE, TILE), TILE)] = block
        base += count * RING
    hot = lax.broadcasted_iota(jnp.int32, y.shape, 0) + where[AT_ROW]
    y[...] = (lax.broadcasted_iota(jnp.int32, y.shape, 1) == hot).astype(jnp.float32)
    eliminate(ks, w, y, tile)


def next_kernel(ks, w_in, y_in, w, y, tile):
    w[...] = w_in[...]
    y[...] = y_in[...]
    eliminate(ks, w, y, tile)


def last_kernel(ks, w_in, y_in, w, x, y, tile):
    w[...] = w_in[...]
    y[...] = y_in[...]
    eliminate(ks, w, y, tile)
    substitute_back(w, y, x)


FACTOR_FLOPS = 400_000_000


def factor_first(ks, where, shift, pieces, width, rows):
    table = jnp.asarray(np.array(upper(width // TILE), np.int32).T)
    outs = [
        jax.ShapeDtypeStruct((width, width), jnp.float32),
        jax.ShapeDtypeStruct((rows, width), jnp.float32),
    ]
    return call(
        functools.partial(first_kernel, ks),
        "factor_first",
        outs,
        [SMEM, SMEM, SMEM] + [VMEM] * len(pieces),
        [pltpu.VMEM((TILE, TILE), jnp.float32)],
        FACTOR_FLOPS * len(ks),
    )(where, shift, table, *pieces)


def factor_next(ks, w, y, last=False):
    outs = [jax.ShapeDtypeStruct(w.shape, w.dtype), jax.ShapeDtypeStruct(y.shape, y.dtype)]
    scratch = [pltpu.VMEM((TILE, TILE), jnp.float32)]
    if last:
        scratch = [pltpu.VMEM(y.shape, y.dtype)] + scratch
    return call(
        functools.partial(last_kernel if last else next_kernel, ks),
        "factor_last" if last else "factor_next",
        outs,
        [VMEM, VMEM],
        scratch,
        FACTOR_FLOPS * len(ks),
    )(w, y)


def left_kernel(where, x, kept, *refs):
    pieces, (slab, low, part) = refs[: 2 * RING], refs[2 * RING :]
    tiles = slab.shape[1] // TILE
    for h, at in enumerate((AT_X, AT_Y)):
        count = pieces[h * RING].shape[0] // TILE
        for s in range(RING):
            chunk = plus(where[at], -s)
            for b in range(count):
                n = (h * RING + chunk) * count + b
                i, j = n // tiles, lax.rem(n, tiles)
                rows = pl.ds(pl.multiple_of(i * TILE, TILE), TILE)
                slab[rows, pl.ds(pl.multiple_of(j * TILE, TILE), TILE)] = pieces[
                    h * RING + s
                ][b * TILE : (b + 1) * TILE, :]
    fresh = where[AT_FRESH] != 0
    low[...] = jnp.where(fresh, x[...].astype(low.dtype), kept[...])
    half = slab.shape[0]
    side = where[AT_SIDE]
    part[...] = jnp.dot(
        low[:, pl.ds(pl.multiple_of(side * half, half), half)],
        slab[...],
        preferred_element_type=jnp.float32,
    )


def left_product(where, x, kept, pieces):
    rows, width = x.shape
    outs = [
        jax.ShapeDtypeStruct((width // 2, width), jnp.bfloat16),
        jax.ShapeDtypeStruct((rows, width), jnp.bfloat16),
        jax.ShapeDtypeStruct((rows, width), jnp.float32),
    ]
    return call(left_kernel, "left_product", outs, [SMEM] + [VMEM] * (2 + len(pieces)))(
        where, x, kept, *pieces
    )


def right_kernel(where, step, w, slab, low, part, kept, out, y, x, held):
    half = slab.shape[0]
    y[...] = part[...] + jnp.dot(low[...], slab[...], preferred_element_type=jnp.float32)
    fresh = where[AT_FRESH] != 0
    tiles = w.shape[0] // TILE

    @pl.when(fresh)
    def _():
        for k in range(tiles - 1):
            start, lo = k * TILE, (k + 1) * TILE
            y[:, lo:] -= dot(y[:, start:lo], w[start:lo, lo:])
        substitute_back(w, y, x)

    @pl.when(jnp.logical_not(fresh))
    def _():
        pltpu.sync_copy(kept, held)
        x[...] = dot(y[...], held[...].astype(jnp.float32))

    out[...] = (x[...] * step[0]).astype(out.dtype)


def right_solve(where, step, w, slab, low, part, kept):
    shape = part.shape
    return call(
        right_kernel,
        "right_solve",
        jax.ShapeDtypeStruct(shape, jnp.bfloat16),
        [SMEM, SMEM] + [VMEM] * 4 + [pl.BlockSpec(memory_space=pl.ANY)],
        [
            pltpu.VMEM(shape, jnp.float32),
            pltpu.VMEM(shape, jnp.float32),
            pltpu.VMEM(kept.shape, kept.dtype),
        ],
    )(where, step, w, slab, low, part, kept)


def tie(*trees):
    return lax.optimization_barrier(trees)


def body(layer_inputs, out_grads, damping, owners, old_inverse, step_size):
    y, z, x = lax.axis_index("y"), lax.axis_index("zh"), lax.axis_index("x")
    layer, side = lax.axis_index("zl"), lax.axis_index("core")
    parts = RING**3
    width = layer_inputs.shape[2]
    rows = width // parts
    scale = 1.0 / (layer_inputs.shape[1] * parts)
    device = (y * RING + z) * RING + x
    factor_id = 2 * layer + side
    fresh = owners[factor_id] < parts
    where = jnp.stack([x, y, z, layer, side, device * rows, fresh.astype(jnp.int32)])
    where = where.astype(jnp.int32)
    shift = damping[factor_id][None]
    step = step_size[layer][None]
    kept = old_inverse[0]
    kept_rows = lax.dynamic_slice_in_dim(kept, device * rows, rows, 0)

    pieces = local_stats(where, layer_inputs, out_grads, (5, 4, 4, 4))
    a0, a1, g0, g1 = (pieces[i * RING : (i + 1) * RING] for i in range(4))

    a0, a1 = split_sum(where, (swap(a0, "x"), swap(a1, "y")), (AT_Y, AT_X), "split_1")
    a0, a1 = split_sum(where, (swap(a0, "y"), swap(a1, "x")), (AT_Z, AT_Z), "split_2")
    a0, a1 = total((swap(a0, "zh"), swap(a1, "zh")), scale, jnp.float32, "total_a")
    a0, a1 = place(where, (spread(a0, "zh"), spread(a1, "zh")), (AT_Z, AT_Z), "place_1")
    a0, a1 = place(where, (spread(a0, "y"), spread(a1, "x")), (AT_Y, AT_X), "place_2")
    a0, a1 = spread(a0, "x"), spread(a1, "y")

    (a0, a1), g0, g1 = tie((a0, a1), g0, g1)
    g0, g1 = swap(g0, "x"), swap(g1, "y")
    w, v = factor_first((0, 1, 2), where, shift, a0 + a1, width, rows)
    g0, g1 = split_sum(where, (g0, g1), (AT_Y, AT_X), "split_3")
    w, v, g0, g1 = tie(w, v, g0, g1)
    g0, g1 = swap(g0, "y"), swap(g1, "x")
    w, v = factor_next((3,), w, v)
    g0, g1 = split_sum(where, (g0, g1), (AT_Z, AT_Z), "split_4")
    w, v, g0, g1 = tie(w, v, g0, g1)
    g0, g1 = swap(g0, "zh"), swap(g1, "zh")
    w, v = factor_next((4,), w, v)
    g0, g1 = total((g0, g1), scale, jnp.bfloat16, "total_g")
    w, v, g0, g1 = tie(w, v, g0, g1)
    g0, g1 = spread(g0, "zh"), spread(g1, "zh")
    w, v = factor_next((5,), w, v)
    g0, g1 = place(where, (g0, g1), (AT_Z, AT_Z), "place_3")
    w, v, g0, g1 = tie(w, v, g0, g1)
    g0, g1 = spread(g0, "y"), spread(g1, "x")
    w, v = factor_next((6,), w, v)
    g0, g1 = place(where, (g0, g1), (AT_Y, AT_X), "place_4")
    w, v, g0, g1 = tie(w, v, g0, g1)
    g0, g1 = spread(g0, "x"), spread(g1, "y")
    w, v = factor_next((7,), w, v, last=True)

    slab, low, part = left_product(where, v, kept_rows, g0 + g1)
    to_input_side = [(1, 0)]
    low = lax.ppermute(low[:, : width // 2], "core", to_input_side)
    part = lax.ppermute(part, "core", to_input_side)
    mine = right_solve(where, step, w, slab, low, part, kept)
    every = lax.all_gather(mine, ("zl", "core"), axis=0)
    return every[0::2]


def solution(mesh):
    split = Mesh(mesh.devices.reshape(RING, RING, RING, 2, 2), ("y", "zh", "x", "zl", "core"))
    tokens = P(None, ("y", "zh", "x"), None)
    placed = (tokens, tokens, P(), P(), P(("zl", "core"), None, None), P())
    return jax.shard_map(
        body, mesh=split, in_specs=placed, out_specs=tokens, check_vma=False
    )
```

```python
import functools

import jax
import jax.numpy as jnp
import numpy as np
from jax import lax
from jax.experimental import pallas as pl
from jax.experimental.pallas import tpu as pltpu
from jax.sharding import Mesh
from jax.sharding import PartitionSpec as P


RING = 4
TILE = 128
HIGHEST = lax.Precision.HIGHEST
VMEM = pl.BlockSpec(memory_space=pltpu.VMEM)
SMEM = pl.BlockSpec(memory_space=pltpu.SMEM)
AT_X, AT_Y, AT_Z, AT_LAYER, AT_SIDE, AT_FRESH = range(6)


def params(mib):
    return pltpu.CompilerParams(vmem_limit_bytes=mib << 20)


def call(kernel, name, out_shape, in_specs, scratch=(), flops=0, aliases=None, mib=4):
    return pl.pallas_call(
        kernel,
        out_shape=out_shape,
        in_specs=in_specs,
        out_specs=jax.tree.map(lambda _: VMEM, out_shape),
        scratch_shapes=scratch,
        compiler_params=params(mib),
        cost_estimate=pl.CostEstimate(flops=flops, transcendentals=0, bytes_accessed=0),
        input_output_aliases=aliases or {},
        name=name,
    )


def upper(tiles):
    return [(i, j) for i in range(tiles) for j in range(i, tiles)]


def plus(coordinate, shift):
    return lax.rem(coordinate + shift + RING, RING)


A_ROWS = (40, 32)
GRAD_ROWS = 32
CHUNK = tuple(a + GRAD_ROWS for a in A_ROWS)


def stats_kernel(where, inputs, grads, *refs):
    outs, (source, factor, slab) = refs[:-3], refs[-3:]
    width = inputs.shape[1]
    tiles = width // TILE
    side = where[AT_SIDE]

    @pl.when(side == 0)
    def _():
        source[...] = inputs[...]

    @pl.when(side != 0)
    def _():
        source[...] = grads[...]

    contract = (((0,), (0,)), ((), ()))
    n = 0
    for i in range(tiles):
        rows = lax.dot_general(
            source[:, i * TILE : (i + 1) * TILE],
            source[:, i * TILE :],
            contract,
            preferred_element_type=jnp.float32,
        )
        for j in range(tiles - i):
            factor[n * TILE : (n + 1) * TILE, :] = rows[:, j * TILE : (j + 1) * TILE]
            n += 1
    half = width // 2
    mine = grads[:, pl.ds(pl.multiple_of(side * half, half), half)]
    slab[...] = lax.dot_general(inputs[...], mine, contract, preferred_element_type=jnp.float32)
    own = width // RING**3
    for h, at in enumerate((AT_X, AT_Y)):
        base = 0 if h == 0 else A_ROWS[0] * RING**3
        to_x, to_y = (1, 16) if h == 0 else (16, 1)
        for shift in range(RING):
            out = outs[h * RING + shift]
            chunk = plus(where[at], shift)
            for second in range(RING):
                for z in range(RING):
                    piece = second * RING + z
                    o = piece * CHUNK[h]
                    at_a = base + (chunk * RING * RING + piece) * A_ROWS[h]
                    out[o : o + A_ROWS[h], :] = factor[
                        pl.ds(pl.multiple_of(at_a, 8), A_ROWS[h]), :
                    ]
                    device = chunk * to_x + second * to_y + z * RING
                    at_g = pl.ds(pl.multiple_of(device * own, 16), own)
                    for b in range(GRAD_ROWS // own):
                        lanes = (h * (GRAD_ROWS // own) + b) * TILE
                        to = o + A_ROWS[h] + b * own
                        out[to : to + own, :] = slab[at_g, lanes : lanes + TILE]


def local_stats(where, inputs, grads):
    _, tokens, width = inputs.shape
    tiles = width // TILE
    outs = [
        jax.ShapeDtypeStruct((c * RING * RING, TILE), jnp.float32)
        for c in CHUNK
        for _ in range(RING)
    ]
    pick = pl.BlockSpec((None, tokens, width), lambda i, where: (where[AT_LAYER], 0, 0))
    return pl.pallas_call(
        stats_kernel,
        out_shape=outs,
        grid_spec=pltpu.PrefetchScalarGridSpec(
            num_scalar_prefetch=1,
            grid=(1,),
            in_specs=[pick, pick],
            out_specs=[pl.BlockSpec(o.shape, lambda i, where: (0, 0)) for o in outs],
            scratch_shapes=[
                pltpu.VMEM((tokens, width), inputs.dtype),
                pltpu.VMEM((len(upper(tiles)) * TILE, TILE), jnp.float32),
                pltpu.VMEM((width, width // 2), jnp.float32),
            ],
        ),
        compiler_params=params(24),
        name="local_stats",
    )(where, inputs, grads)


def four(parts):
    return (parts[0] + parts[1]) + (parts[2] + parts[3])


def sum_kernel(*refs):
    for h, out in enumerate(refs[-2:]):
        out[...] = four([ref[...] for ref in refs[h * RING : (h + 1) * RING]])


def sum_parts(halves):
    flat = [a for half in halves for a in half]
    outs = [jax.ShapeDtypeStruct(half[0].shape, jnp.float32) for half in halves]
    return call(sum_kernel, "sum_parts", outs, [VMEM] * len(flat))(*flat)


def join_kernel(a0, a1, out):
    for h, a in enumerate((a0, a1)):
        o = h * CHUNK[0]
        for z in range(RING):
            rows = slice(z * CHUNK[h], (z + 1) * CHUNK[h])
            out[z, o : o + CHUNK[h], :] = four([a[q, rows, :] for q in range(RING)])


def join_halves(a0, a1):
    out = jax.ShapeDtypeStruct((RING, sum(CHUNK), TILE), jnp.float32)
    return call(join_kernel, "join_halves", out, [VMEM, VMEM])(a0, a1)


def total_kernel(scale, parts, a, g):
    o, to = 0, 0
    own = g.shape[0]
    for h in range(2):
        rows = slice(o, o + A_ROWS[h])
        a[to : to + A_ROWS[h], :] = four([parts[q, rows, :] for q in range(RING)]) * scale
        to += A_ROWS[h]
        for b in range(GRAD_ROWS // own):
            at = o + A_ROWS[h] + b * own
            lanes = (h * (GRAD_ROWS // own) + b) * TILE
            value = four([parts[q, at : at + own, :] for q in range(RING)]) * scale
            g[:, lanes : lanes + TILE] = value.astype(g.dtype)
        o += CHUNK[h]


def total(parts, scale, own, width):
    outs = [
        jax.ShapeDtypeStruct((sum(A_ROWS), TILE), jnp.float32),
        jax.ShapeDtypeStruct((own, width // 2), jnp.bfloat16),
    ]
    return call(functools.partial(total_kernel, scale), "total", outs, [VMEM])(parts)


def part_kernel(pieces, *outs):
    for h, out in enumerate(outs):
        o = h * A_ROWS[0]
        for z in range(RING):
            out[z * A_ROWS[h] : (z + 1) * A_ROWS[h], :] = pieces[z, o : o + A_ROWS[h], :]


def part_halves(pieces):
    outs = [jax.ShapeDtypeStruct((a * RING, TILE), jnp.float32) for a in A_ROWS]
    return call(part_kernel, "part_halves", outs, [VMEM])(pieces)


def send(a, axis, shift):
    return lax.ppermute(a, axis, [(i, (i + shift) % RING) for i in range(RING)])


def swap(half, axis):
    return [half[0]] + [send(half[s], axis, s) for s in range(1, RING)]


def spread(a, axis):
    return [a] + [send(a, axis, s) for s in range(1, RING)]


def exchange(a, axis):
    a = a.reshape(RING, a.shape[0] // RING, TILE)
    return lax.all_to_all(a, axis, split_axis=0, concat_axis=0)


def gather(a, axis):
    return lax.all_gather(a, axis, axis=0, tiled=True)


def row_of(x, t):
    return jnp.broadcast_to(x[t : t + 1, :], x.shape)


def column_of(x, t):
    return jnp.broadcast_to(x[:, t : t + 1], x.shape)


def invert_tile(tile):
    lane = lax.broadcasted_iota(jnp.int32, (8, TILE), 1)
    sub = lax.broadcasted_iota(jnp.int32, (8, TILE), 0)
    for start in range(0, TILE, 8):
        inside = (lane >= start) & (lane < start + 8)
        rows = tile[start : start + 8, :]
        columns = [column_of(rows, start + t) for t in range(8)]
        strip = jnp.where(inside, (lane - start == sub).astype(jnp.float32), rows)
        for t in range(8):
            here = sub == t
            pivot = 1.0 / row_of(columns[t], t)
            for j in range(t + 1, 8):
                r = row_of(columns[j], t) * pivot
                columns[j] = jnp.where(here, r, columns[j] - columns[t] * r)
            r = row_of(strip, t) * pivot
            strip = jnp.where(here, r, strip - columns[t] * r)
        pivots = [row_of(strip, t) for t in range(8)]
        for other in range(0, TILE, 8):
            if other != start:
                block = tile[other : other + 8, :]
                left = jnp.where(inside, 0.0, block)
                for t in range(8):
                    left = left - column_of(block, start + t) * pivots[t]
                tile[other : other + 8, :] = left
        tile[start : start + 8, :] = strip


def dot(a, b):
    return jnp.dot(a, b, preferred_element_type=jnp.float32, precision=HIGHEST)


def eliminate(ks, w, y, tile):
    tiles = w.shape[0] // TILE

    def step(k, carry):
        here = pl.ds(pl.multiple_of(k * TILE, TILE), TILE)
        tile[...] = w[here, here]
        invert_tile(tile)
        w[here, here] = tile[...]
        for kk in ks:
            if kk < tiles - 1:

                @pl.when(k == kk)
                def _():
                    start, lo = kk * TILE, (kk + 1) * TILE
                    panel = w[start:lo, lo:]
                    scaled = dot(tile[...], panel)
                    w[start:lo, lo:] = scaled
                    y[:, lo:] -= dot(y[:, start:lo], scaled)
                    turned = panel.T
                    for i in range(kk + 1, tiles):
                        o = (i - kk - 1) * TILE
                        w[i * TILE : (i + 1) * TILE, i * TILE :] -= dot(
                            turned[o : o + TILE, :], scaled[:, o:]
                        )

        return carry

    lax.fori_loop(ks[0], ks[-1] + 1, step, 0)


def substitute_back(w, y, x):
    tiles = w.shape[0] // TILE
    for k in range(tiles):
        c = slice(k * TILE, (k + 1) * TILE)
        x[:, c] = dot(y[:, c], w[c, c])
    for k in reversed(range(tiles - 1)):
        c, lo = slice(k * TILE, (k + 1) * TILE), (k + 1) * TILE
        x[:, c] -= lax.dot_general(
            x[:, lo:],
            w[c, lo:],
            (((1,), (1,)), ((), ())),
            preferred_element_type=jnp.float32,
            precision=HIGHEST,
        )


def fill(where, shift, table, pieces, w):
    line = lax.broadcasted_iota(jnp.int32, (TILE, TILE), 0)
    damp = jnp.where(line == lax.broadcasted_iota(jnp.int32, (TILE, TILE), 1), shift[0], 0.0)
    base = 0
    for h, at in enumerate((AT_X, AT_Y)):
        count = pieces[h * RING].shape[0] // TILE
        for s in range(RING):
            for b in range(count):
                n = base + plus(where[at], -s) * count + b
                i, j = table[0, n], table[1, n]
                block = pieces[h * RING + s][b * TILE : (b + 1) * TILE, :]
                block = block + jnp.where(i == j, 1.0, 0.0) * damp
                rows = pl.ds(pl.multiple_of(i * TILE, TILE), TILE)
                w[rows, pl.ds(pl.multiple_of(j * TILE, TILE), TILE)] = block
        base += count * RING


def times_kept(kept, held, y, x):
    pltpu.sync_copy(kept, held)
    x[...] = dot(y[...], held[...].astype(jnp.float32))


def left_kernel(where, shift, table, low, high, kept, *refs):
    pieces, (w, x, y, tile, held) = refs[: 2 * RING], refs[2 * RING :]
    half = low.shape[1]
    y[:, :half] = low[...].astype(y.dtype)
    y[:, half:] = high[...].astype(y.dtype)
    fresh = where[AT_FRESH] != 0

    @pl.when(fresh)
    def _():
        fill(where, shift, table, pieces, w)
        eliminate(range(w.shape[0] // TILE), w, y, tile)
        substitute_back(w, y, x)

    @pl.when(jnp.logical_not(fresh))
    def _():
        times_kept(kept, held, y, x)


def left_solve(where, shift, pieces, low, high, kept):
    rows, width = low.shape[0], kept.shape[0]
    table = jnp.asarray(np.array(upper(width // TILE), np.int32).T)
    outs = [
        jax.ShapeDtypeStruct((width, width), jnp.float32),
        jax.ShapeDtypeStruct((rows, width), jnp.float32),
    ]
    return call(
        left_kernel,
        "left_solve",
        outs,
        [SMEM, SMEM, SMEM, VMEM, VMEM, pl.BlockSpec(memory_space=pl.ANY)]
        + [VMEM] * len(pieces),
        [
            pltpu.VMEM((rows, width), jnp.float32),
            pltpu.VMEM((TILE, TILE), jnp.float32),
            pltpu.VMEM(kept.shape, kept.dtype),
        ],
        3_000_000_000,
        mib=12,
    )(where, shift, table, low, high, kept, *pieces)


def right_kernel(where, step, w, b, kept, out, y, x, held):
    fresh = where[AT_FRESH] != 0
    tiles = w.shape[0] // TILE
    y[...] = b[...]

    @pl.when(fresh)
    def _():
        for k in range(tiles - 1):
            start, lo = k * TILE, (k + 1) * TILE
            y[:, lo:] -= dot(y[:, start:lo], w[start:lo, lo:])
        substitute_back(w, y, x)

    @pl.when(jnp.logical_not(fresh))
    def _():
        times_kept(kept, held, y, x)

    out[...] = (x[...] * step[0]).astype(out.dtype)


def right_solve(where, step, w, b, kept):
    return call(
        right_kernel,
        "right_solve",
        jax.ShapeDtypeStruct(b.shape, jnp.bfloat16),
        [SMEM, SMEM, VMEM, VMEM, pl.BlockSpec(memory_space=pl.ANY)],
        [
            pltpu.VMEM(b.shape, jnp.float32),
            pltpu.VMEM(b.shape, jnp.float32),
            pltpu.VMEM(kept.shape, kept.dtype),
        ],
        mib=12,
    )(where, step, w, b, kept)


def body(layer_inputs, out_grads, damping, owners, old_inverse, step_size):
    y, z, x = lax.axis_index("y"), lax.axis_index("zh"), lax.axis_index("x")
    layer, side = lax.axis_index("zl"), lax.axis_index("core")
    parts = RING**3
    width = layer_inputs.shape[2]
    own = width // parts
    scale = 1.0 / (layer_inputs.shape[1] * parts)
    factor_id = 2 * layer + side
    fresh = owners[factor_id] < parts
    where = jnp.stack([x, y, z, layer, side, fresh.astype(jnp.int32)]).astype(jnp.int32)
    shift = damping[factor_id][None]
    step = step_size[layer][None]
    kept = old_inverse[0]

    pieces = local_stats(where, layer_inputs, out_grads)
    a0, a1 = sum_parts((swap(pieces[:RING], "x"), swap(pieces[RING:], "y")))
    both = join_halves(exchange(a0, "y"), exchange(a1, "x"))
    both = lax.all_to_all(both, "zh", split_axis=0, concat_axis=0)
    a, high = total(both, scale, own, width)
    low = lax.ppermute(high, "core", [(0, 1)])
    a0, a1 = part_halves(lax.all_gather(a, "zh", axis=0))
    a0, a1 = spread(gather(a0, "y"), "x"), spread(gather(a1, "x"), "y")

    w, v = left_solve(where, shift, a0 + a1, low, high, kept)
    v = v.reshape(own, parts, own).transpose(1, 0, 2).reshape(parts, own * own // TILE, TILE)
    v = lax.ppermute(v, "core", [(1, 0)])
    v = lax.all_to_all(v, ("y", "zh", "x"), split_axis=0, concat_axis=0)
    v = v.reshape(parts * own, own).T
    mine = right_solve(where, step, w, v, kept)
    every = lax.all_gather(mine, ("zl", "core"), axis=0)
    return every[0::2]


def solution(mesh):
    split = Mesh(mesh.devices.reshape(RING, RING, RING, 2, 2), ("y", "zh", "x", "zl", "core"))
    tokens = P(None, ("y", "zh", "x"), None)
    placed = (tokens, tokens, P(), P(), P(("zl", "core"), None, None), P())
    return jax.shard_map(
        body, mesh=split, in_specs=placed, out_specs=tokens, check_vma=False
    )
```

```python
import functools

import jax
import jax.numpy as jnp
import numpy as np
from jax import lax
from jax.experimental import pallas as pl
from jax.experimental.pallas import tpu as pltpu
from jax.sharding import Mesh
from jax.sharding import PartitionSpec as P


RING = 4
TILE = 128
HIGHEST = lax.Precision.HIGHEST
VMEM = pl.BlockSpec(memory_space=pltpu.VMEM)
SMEM = pl.BlockSpec(memory_space=pltpu.SMEM)
AT_X, AT_Y, AT_Z, AT_LAYER, AT_SIDE, AT_FRESH = range(6)


def params(mib):
    return pltpu.CompilerParams(vmem_limit_bytes=mib << 20)


def call(kernel, name, out_shape, in_specs, scratch=(), flops=0, aliases=None, mib=4):
    return pl.pallas_call(
        kernel,
        out_shape=out_shape,
        in_specs=in_specs,
        out_specs=jax.tree.map(lambda _: VMEM, out_shape),
        scratch_shapes=scratch,
        compiler_params=params(mib),
        cost_estimate=pl.CostEstimate(flops=flops, transcendentals=0, bytes_accessed=0),
        input_output_aliases=aliases or {},
        name=name,
    )


def upper(tiles):
    return [(i, j) for i in range(tiles) for j in range(i, tiles)]


def plus(coordinate, shift):
    return lax.rem(coordinate + shift + RING, RING)


A_ROWS = (40, 32)
GRAD_ROWS = 32
CHUNK = tuple(a + GRAD_ROWS for a in A_ROWS)


def stats_kernel(where, inputs, grads, *refs):
    outs, (source, factor, slab) = refs[:-3], refs[-3:]
    width = inputs.shape[1]
    tiles = width // TILE
    side = where[AT_SIDE]

    @pl.when(side == 0)
    def _():
        source[...] = inputs[...]

    @pl.when(side != 0)
    def _():
        source[...] = grads[...]

    contract = (((0,), (0,)), ((), ()))
    n = 0
    for i in range(tiles):
        rows = lax.dot_general(
            source[:, i * TILE : (i + 1) * TILE],
            source[:, i * TILE :],
            contract,
            preferred_element_type=jnp.float32,
        )
        for j in range(tiles - i):
            factor[n * TILE : (n + 1) * TILE, :] = rows[:, j * TILE : (j + 1) * TILE]
            n += 1
    half = width // 2
    mine = grads[:, pl.ds(pl.multiple_of(side * half, half), half)]
    slab[...] = lax.dot_general(inputs[...], mine, contract, preferred_element_type=jnp.float32)
    own = width // RING**3
    for h, at in enumerate((AT_X, AT_Y)):
        base = 0 if h == 0 else A_ROWS[0] * RING**3
        to_x, to_y = (1, 16) if h == 0 else (16, 1)
        for shift in range(RING):
            out = outs[h * RING + shift]
            chunk = plus(where[at], shift)
            for second in range(RING):
                for z in range(RING):
                    piece = second * RING + z
                    o = piece * CHUNK[h]
                    at_a = base + (chunk * RING * RING + piece) * A_ROWS[h]
                    out[o : o + A_ROWS[h], :] = factor[
                        pl.ds(pl.multiple_of(at_a, 8), A_ROWS[h]), :
                    ]
                    device = chunk * to_x + second * to_y + z * RING
                    at_g = pl.ds(pl.multiple_of(device * own, 16), own)
                    for b in range(GRAD_ROWS // own):
                        lanes = (h * (GRAD_ROWS // own) + b) * TILE
                        to = o + A_ROWS[h] + b * own
                        out[to : to + own, :] = slab[at_g, lanes : lanes + TILE]


def local_stats(where, inputs, grads):
    _, tokens, width = inputs.shape
    tiles = width // TILE
    outs = [
        jax.ShapeDtypeStruct((c * RING * RING, TILE), jnp.float32)
        for c in CHUNK
        for _ in range(RING)
    ]
    pick = pl.BlockSpec((None, tokens, width), lambda i, where: (where[AT_LAYER], 0, 0))
    return pl.pallas_call(
        stats_kernel,
        out_shape=outs,
        grid_spec=pltpu.PrefetchScalarGridSpec(
            num_scalar_prefetch=1,
            grid=(1,),
            in_specs=[pick, pick],
            out_specs=[pl.BlockSpec(o.shape, lambda i, where: (0, 0)) for o in outs],
            scratch_shapes=[
                pltpu.VMEM((tokens, width), inputs.dtype),
                pltpu.VMEM((len(upper(tiles)) * TILE, TILE), jnp.float32),
                pltpu.VMEM((width, width // 2), jnp.float32),
            ],
        ),
        compiler_params=params(24),
        name="local_stats",
    )(where, inputs, grads)


def four(parts):
    return (parts[0] + parts[1]) + (parts[2] + parts[3])


def split_kernel(ats, where, *refs):
    for h, at in enumerate(ats):
        ins = refs[h * RING : (h + 1) * RING]
        outs = refs[(len(ats) + h) * RING : (len(ats) + h + 1) * RING]
        rows = outs[0].shape[0]
        for shift in range(RING):
            part = pl.ds(pl.multiple_of(plus(where[at], shift) * rows, 8), rows)
            outs[shift][...] = four([ref[part, :] for ref in ins])


def split_sum(where, halves, ats):
    flat = [a for half in halves for a in half]
    outs = [jax.ShapeDtypeStruct((a.shape[0] // RING, TILE), a.dtype) for a in flat]
    kernel = functools.partial(split_kernel, ats)
    got = call(kernel, "split_sum", outs, [SMEM] + [VMEM] * len(flat))(where, *flat)
    return got[:RING], got[RING:]


def join_kernel(where, *refs):
    for shift, out in enumerate(refs[2 * RING :]):
        chunk = plus(where[AT_Z], shift)
        o = 0
        for h, rows in enumerate(CHUNK):
            part = pl.ds(pl.multiple_of(chunk * rows, 8), rows)
            ins = refs[h * RING : (h + 1) * RING]
            out[o : o + rows, :] = four([ref[part, :] for ref in ins])
            o += rows


def join_sum(where, halves):
    flat = [a for half in halves for a in half]
    outs = [jax.ShapeDtypeStruct((sum(CHUNK), TILE), jnp.float32)] * RING
    return call(join_kernel, "join_sum", outs, [SMEM] + [VMEM] * len(flat))(where, *flat)


def total_kernel(scale, *refs):
    parts, (a, g) = refs[:-2], refs[-2:]
    o, to = 0, 0
    own = g.shape[0]
    for h in range(2):
        rows = slice(o, o + A_ROWS[h])
        a[to : to + A_ROWS[h], :] = four([part[rows, :] for part in parts]) * scale
        to += A_ROWS[h]
        for b in range(GRAD_ROWS // own):
            at = o + A_ROWS[h] + b * own
            lanes = (h * (GRAD_ROWS // own) + b) * TILE
            value = four([part[at : at + own, :] for part in parts]) * scale
            g[:, lanes : lanes + TILE] = value.astype(g.dtype)
        o += CHUNK[h]


def total(parts, scale, own, width):
    outs = [
        jax.ShapeDtypeStruct((sum(A_ROWS), TILE), jnp.float32),
        jax.ShapeDtypeStruct((own, width // 2), jnp.bfloat16),
    ]
    kernel = functools.partial(total_kernel, scale)
    return call(kernel, "total", outs, [VMEM] * RING)(*parts)


def part_kernel(where, *refs):
    outs = refs[RING:]
    for shift in range(RING):
        chunk = plus(where[AT_Z], -shift)
        o = 0
        for out, rows in zip(outs, A_ROWS):
            to = pl.ds(pl.multiple_of(chunk * rows, 8), rows)
            out[to, :] = refs[shift][o : o + rows, :]
            o += rows


def part_halves(where, pieces):
    outs = [jax.ShapeDtypeStruct((a * RING, TILE), jnp.float32) for a in A_ROWS]
    return call(part_kernel, "part_halves", outs, [SMEM] + [VMEM] * RING)(where, *pieces)


def place_kernel(ats, where, *refs):
    for h, at in enumerate(ats):
        out = refs[len(ats) * RING + h]
        for shift in range(RING):
            piece = refs[h * RING + shift]
            rows = piece.shape[0]
            to = pl.multiple_of(plus(where[at], -shift) * rows, 8)
            out[pl.ds(to, rows), :] = piece[...]


def place(where, halves, ats):
    flat = [a for half in halves for a in half]
    outs = [jax.ShapeDtypeStruct((half[0].shape[0] * RING, TILE), jnp.float32) for half in halves]
    kernel = functools.partial(place_kernel, ats)
    return call(kernel, "place", outs, [SMEM] + [VMEM] * len(flat))(where, *flat)


def send(a, axis, shift):
    return lax.ppermute(a, axis, [(i, (i + shift) % RING) for i in range(RING)])


def swap(half, axis):
    return [half[0]] + [send(half[s], axis, s) for s in range(1, RING)]


def spread(a, axis):
    return [a] + [send(a, axis, s) for s in range(1, RING)]


def row_of(x, t):
    return jnp.broadcast_to(x[t : t + 1, :], x.shape)


def column_of(x, t):
    return jnp.broadcast_to(x[:, t : t + 1], x.shape)


def inverse_of(x):
    guess = pltpu.reciprocal(x, approx=True)
    return guess * (2.0 - x * guess)


def invert_tile(tile):
    lane = lax.broadcasted_iota(jnp.int32, (8, TILE), 1)
    sub = lax.broadcasted_iota(jnp.int32, (8, TILE), 0)
    rows = tile[0:8, :]
    columns = [column_of(rows, t) for t in range(8)]
    for start in range(0, TILE, 8):
        inside = (lane >= start) & (lane < start + 8)
        strip = jnp.where(inside, (lane - start == sub).astype(jnp.float32), rows)
        scale = strip
        for t in range(8):
            here = sub == t
            pivot = inverse_of(row_of(columns[t], t))
            scale = jnp.where(here, pivot, scale)
            ratio = jnp.where(here, 0.0, columns[t]) * pivot
            for j in range(t + 1, 8):
                columns[j] = columns[j] - ratio * row_of(columns[j], t)
            strip = strip - ratio * row_of(strip, t)
        strip = strip * scale
        pivots = [row_of(strip, t) for t in range(8)]
        later = list(range(start + 8, TILE, 8)) + list(range(0, start, 8))
        for other in later:
            block = tile[other : other + 8, :]
            left = jnp.where(inside, 0.0, block)
            for t in range(8):
                left = left - column_of(block, start + t) * pivots[t]
            tile[other : other + 8, :] = left
            if other == start + 8:
                rows = left
                columns = [column_of(rows, other + t) for t in range(8)]
        tile[start : start + 8, :] = strip


def dot(a, b):
    return jnp.dot(a, b, preferred_element_type=jnp.float32, precision=HIGHEST)


def eliminate(ks, w, y, tile):
    tiles = w.shape[0] // TILE

    def step(k, carry):
        here = pl.ds(pl.multiple_of(k * TILE, TILE), TILE)
        tile[...] = w[here, here]
        invert_tile(tile)
        w[here, here] = tile[...]
        for kk in ks:
            if kk < tiles - 1:

                @pl.when(k == kk)
                def _():
                    start, lo = kk * TILE, (kk + 1) * TILE
                    panel = w[start:lo, lo:]
                    scaled = dot(tile[...], panel)
                    w[start:lo, lo:] = scaled
                    y[:, lo:] -= dot(y[:, start:lo], scaled)
                    turned = panel.T
                    for i in range(kk + 1, tiles):
                        o = (i - kk - 1) * TILE
                        w[i * TILE : (i + 1) * TILE, i * TILE :] -= dot(
                            turned[o : o + TILE, :], scaled[:, o:]
                        )

        return carry

    lax.fori_loop(ks[0], ks[-1] + 1, step, 0)


def substitute_back(w, y, x):
    tiles = w.shape[0] // TILE
    for k in range(tiles):
        c = slice(k * TILE, (k + 1) * TILE)
        x[:, c] = dot(y[:, c], w[c, c])
    for k in reversed(range(tiles - 1)):
        c, lo = slice(k * TILE, (k + 1) * TILE), (k + 1) * TILE
        x[:, c] -= lax.dot_general(
            x[:, lo:],
            w[c, lo:],
            (((1,), (1,)), ((), ())),
            preferred_element_type=jnp.float32,
            precision=HIGHEST,
        )


def fill(where, shift, table, pieces, w):
    line = lax.broadcasted_iota(jnp.int32, (TILE, TILE), 0)
    damp = jnp.where(line == lax.broadcasted_iota(jnp.int32, (TILE, TILE), 1), shift[0], 0.0)
    base = 0
    for h, at in enumerate((AT_X, AT_Y)):
        count = pieces[h * RING].shape[0] // TILE
        for s in range(RING):
            for b in range(count):
                n = base + plus(where[at], -s) * count + b
                i, j = table[0, n], table[1, n]
                block = pieces[h * RING + s][b * TILE : (b + 1) * TILE, :]
                block = block + jnp.where(i == j, 1.0, 0.0) * damp
                rows = pl.ds(pl.multiple_of(i * TILE, TILE), TILE)
                w[rows, pl.ds(pl.multiple_of(j * TILE, TILE), TILE)] = block
        base += count * RING


def times_kept(kept, held, y, x):
    pltpu.sync_copy(kept, held)
    x[...] = dot(y[...], held[...].astype(jnp.float32))


def left_kernel(where, shift, table, low, high, kept, *refs):
    pieces, (w, x, y, tile, held) = refs[: 2 * RING], refs[2 * RING :]
    half = low.shape[1]
    y[:, :half] = low[...].astype(y.dtype)
    y[:, half:] = high[...].astype(y.dtype)
    fresh = where[AT_FRESH] != 0

    @pl.when(fresh)
    def _():
        fill(where, shift, table, pieces, w)
        eliminate(range(w.shape[0] // TILE), w, y, tile)
        substitute_back(w, y, x)

    @pl.when(jnp.logical_not(fresh))
    def _():
        times_kept(kept, held, y, x)


def left_solve(where, shift, pieces, low, high, kept):
    rows, width = low.shape[0], kept.shape[0]
    table = jnp.asarray(np.array(upper(width // TILE), np.int32).T)
    outs = [
        jax.ShapeDtypeStruct((width, width), jnp.float32),
        jax.ShapeDtypeStruct((rows, width), jnp.float32),
    ]
    return call(
        left_kernel,
        "left_solve",
        outs,
        [SMEM, SMEM, SMEM, VMEM, VMEM, pl.BlockSpec(memory_space=pl.ANY)]
        + [VMEM] * len(pieces),
        [
            pltpu.VMEM((rows, width), jnp.float32),
            pltpu.VMEM((TILE, TILE), jnp.float32),
            pltpu.VMEM(kept.shape, kept.dtype),
        ],
        3_000_000_000,
        mib=12,
    )(where, shift, table, low, high, kept, *pieces)


def right_kernel(where, step, w, b, kept, out, y, x, held):
    fresh = where[AT_FRESH] != 0
    tiles = w.shape[0] // TILE
    y[...] = b[...]

    @pl.when(fresh)
    def _():
        for k in range(tiles - 1):
            start, lo = k * TILE, (k + 1) * TILE
            y[:, lo:] -= dot(y[:, start:lo], w[start:lo, lo:])
        substitute_back(w, y, x)

    @pl.when(jnp.logical_not(fresh))
    def _():
        times_kept(kept, held, y, x)

    out[...] = (x[...] * step[0]).astype(out.dtype)


def right_solve(where, step, w, b, kept):
    return call(
        right_kernel,
        "right_solve",
        jax.ShapeDtypeStruct(b.shape, jnp.bfloat16),
        [SMEM, SMEM, VMEM, VMEM, pl.BlockSpec(memory_space=pl.ANY)],
        [
            pltpu.VMEM(b.shape, jnp.float32),
            pltpu.VMEM(b.shape, jnp.float32),
            pltpu.VMEM(kept.shape, kept.dtype),
        ],
        mib=12,
    )(where, step, w, b, kept)


def body(layer_inputs, out_grads, damping, owners, old_inverse, step_size):
    y, z, x = lax.axis_index("y"), lax.axis_index("zh"), lax.axis_index("x")
    layer, side = lax.axis_index("zl"), lax.axis_index("core")
    parts = RING**3
    width = layer_inputs.shape[2]
    own = width // parts
    scale = 1.0 / (layer_inputs.shape[1] * parts)
    factor_id = 2 * layer + side
    fresh = owners[factor_id] < parts
    where = jnp.stack([x, y, z, layer, side, fresh.astype(jnp.int32)]).astype(jnp.int32)
    shift = damping[factor_id][None]
    step = step_size[layer][None]
    kept = old_inverse[0]

    pieces = local_stats(where, layer_inputs, out_grads)
    a0, a1 = split_sum(where, (swap(pieces[:RING], "x"), swap(pieces[RING:], "y")), (AT_Y, AT_X))
    both = join_sum(where, (swap(a0, "y"), swap(a1, "x")))
    a, high = total(swap(both, "zh"), scale, own, width)
    a0, a1 = part_halves(where, spread(a, "zh"))
    a0, a1 = place(where, (spread(a0, "y"), spread(a1, "x")), (AT_Y, AT_X))
    a0, a1 = spread(a0, "x"), spread(a1, "y")
    low = lax.ppermute(high, "core", [(0, 1)])

    w, v = left_solve(where, shift, a0 + a1, low, high, kept)
    v = v.reshape(own, parts, own).transpose(1, 0, 2).reshape(parts, own * own // TILE, TILE)
    v = lax.ppermute(v, "core", [(1, 0)])
    v = lax.all_to_all(v, ("y", "zh", "x"), split_axis=0, concat_axis=0)
    v = v.reshape(parts * own, own).T
    mine = right_solve(where, step, w, v, kept)
    every = lax.all_gather(mine, ("zl", "core"), axis=0)
    return every[0::2]


def solution(mesh):
    split = Mesh(mesh.devices.reshape(RING, RING, RING, 2, 2), ("y", "zh", "x", "zl", "core"))
    tokens = P(None, ("y", "zh", "x"), None)
    placed = (tokens, tokens, P(), P(), P(("zl", "core"), None, None), P())
    return jax.shard_map(
        body, mesh=split, in_specs=placed, out_specs=tokens, check_vma=False
    )
```

```python
import functools

import jax
import jax.numpy as jnp
import numpy as np
from jax import lax
from jax.experimental import pallas as pl
from jax.experimental.pallas import tpu as pltpu
from jax.sharding import Mesh
from jax.sharding import PartitionSpec as P


RING = 4
TILE = 128
VMEM = pl.BlockSpec(memory_space=pltpu.VMEM)
SMEM = pl.BlockSpec(memory_space=pltpu.SMEM)
AT_X, AT_Y, AT_Z, AT_LAYER, AT_SIDE = range(5)


def params(mib):
    return pltpu.CompilerParams(vmem_limit_bytes=mib << 20)


def call(kernel, name, out_shape, in_specs, scratch=(), flops=0, aliases=None, mib=4):
    return pl.pallas_call(
        kernel,
        out_shape=out_shape,
        in_specs=in_specs,
        out_specs=jax.tree.map(lambda _: VMEM, out_shape),
        scratch_shapes=scratch,
        compiler_params=params(mib),
        cost_estimate=pl.CostEstimate(flops=flops, transcendentals=0, bytes_accessed=0),
        input_output_aliases=aliases or {},
        name=name,
    )


def upper(tiles):
    return [(i, j) for i in range(tiles) for j in range(i, tiles)]


def plus(coordinate, shift):
    return lax.rem(coordinate + shift + RING, RING)


A_ROWS = (40, 32)
GRAD_ROWS = 32
CHUNK = tuple(a + GRAD_ROWS for a in A_ROWS)


def stats_kernel(where, inputs, grads, *refs):
    outs, (source, factor, slab) = refs[:-3], refs[-3:]
    width = inputs.shape[1]
    tiles = width // TILE
    side = where[AT_SIDE]

    @pl.when(side == 0)
    def _():
        source[...] = inputs[...]

    @pl.when(side != 0)
    def _():
        source[...] = grads[...]

    contract = (((0,), (0,)), ((), ()))
    n = 0
    for i in range(tiles):
        rows = lax.dot_general(
            source[:, i * TILE : (i + 1) * TILE],
            source[:, i * TILE :],
            contract,
            preferred_element_type=jnp.float32,
        )
        for j in range(tiles - i):
            factor[n * TILE : (n + 1) * TILE, :] = rows[:, j * TILE : (j + 1) * TILE]
            n += 1
    half = width // 2
    mine = grads[:, pl.ds(pl.multiple_of(side * half, half), half)]
    slab[...] = lax.dot_general(inputs[...], mine, contract, preferred_element_type=jnp.float32)
    own = width // RING**3
    for h, at in enumerate((AT_X, AT_Y)):
        base = 0 if h == 0 else A_ROWS[0] * RING**3
        to_x, to_y = (1, 16) if h == 0 else (16, 1)
        for shift in range(RING):
            out = outs[h * RING + shift]
            chunk = plus(where[at], shift)
            for second in range(RING):
                for z in range(RING):
                    piece = second * RING + z
                    o = piece * CHUNK[h]
                    at_a = base + (chunk * RING * RING + piece) * A_ROWS[h]
                    out[o : o + A_ROWS[h], :] = factor[
                        pl.ds(pl.multiple_of(at_a, 8), A_ROWS[h]), :
                    ]
                    device = chunk * to_x + second * to_y + z * RING
                    at_g = pl.ds(pl.multiple_of(device * own, 16), own)
                    for b in range(GRAD_ROWS // own):
                        lanes = (h * (GRAD_ROWS // own) + b) * TILE
                        to = o + A_ROWS[h] + b * own
                        out[to : to + own, :] = slab[at_g, lanes : lanes + TILE]


def local_stats(where, inputs, grads):
    _, tokens, width = inputs.shape
    tiles = width // TILE
    outs = [
        jax.ShapeDtypeStruct((c * RING * RING, TILE), jnp.float32)
        for c in CHUNK
        for _ in range(RING)
    ]
    pick = pl.BlockSpec((None, tokens, width), lambda i, where: (where[AT_LAYER], 0, 0))
    return pl.pallas_call(
        stats_kernel,
        out_shape=outs,
        grid_spec=pltpu.PrefetchScalarGridSpec(
            num_scalar_prefetch=1,
            grid=(1,),
            in_specs=[pick, pick],
            out_specs=[pl.BlockSpec(o.shape, lambda i, where: (0, 0)) for o in outs],
            scratch_shapes=[
                pltpu.VMEM((tokens, width), inputs.dtype),
                pltpu.VMEM((len(upper(tiles)) * TILE, TILE), jnp.float32),
                pltpu.VMEM((width, width // 2), jnp.float32),
            ],
        ),
        compiler_params=params(24),
        name="local_stats",
    )(where, inputs, grads)


def four(parts):
    return (parts[0] + parts[1]) + (parts[2] + parts[3])


def split_kernel(ats, where, *refs):
    for h, at in enumerate(ats):
        ins = refs[h * RING : (h + 1) * RING]
        outs = refs[(len(ats) + h) * RING : (len(ats) + h + 1) * RING]
        rows = outs[0].shape[0]
        for shift in range(RING):
            part = pl.ds(pl.multiple_of(plus(where[at], shift) * rows, 8), rows)
            outs[shift][...] = four([ref[part, :] for ref in ins])


def split_sum(where, halves, ats):
    flat = [a for half in halves for a in half]
    outs = [jax.ShapeDtypeStruct((a.shape[0] // RING, TILE), a.dtype) for a in flat]
    kernel = functools.partial(split_kernel, ats)
    got = call(kernel, "split_sum", outs, [SMEM] + [VMEM] * len(flat))(where, *flat)
    return got[:RING], got[RING:]


def join_kernel(where, *refs):
    outs = refs[2 * RING :]
    at = 0
    for h, rows in enumerate(CHUNK):
        ins = refs[h * RING : (h + 1) * RING]
        for z in range(RING):
            o = z * rows
            part = four([ref[o : o + A_ROWS[h], :] for ref in ins])
            for out in outs:
                out[at : at + A_ROWS[h], :] = part
            at += A_ROWS[h]
    for h, rows in enumerate(CHUNK):
        ins = refs[h * RING : (h + 1) * RING]
        for shift, out in enumerate(outs):
            o = pl.multiple_of(plus(where[AT_Z], shift) * rows + A_ROWS[h], 8)
            out[at : at + GRAD_ROWS, :] = four([ref[pl.ds(o, GRAD_ROWS), :] for ref in ins])
        at += GRAD_ROWS


def join_sum(where, halves):
    flat = [a for half in halves for a in half]
    rows = RING * sum(A_ROWS) + 2 * GRAD_ROWS
    outs = [jax.ShapeDtypeStruct((rows, TILE), jnp.float32)] * RING
    return call(join_kernel, "join_sum", outs, [SMEM] + [VMEM] * len(flat))(where, *flat)


def total_kernel(scale, *refs):
    parts, (a0, a1, g) = refs[:RING], refs[RING:]
    o = 0
    own = g.shape[0]
    for a in (a0, a1):
        rows = slice(o, o + a.shape[0])
        a[...] = four([part[rows, :] for part in parts]) * scale
        o += a.shape[0]
    for b in range(2 * GRAD_ROWS // own):
        rows = slice(o + b * own, o + (b + 1) * own)
        value = four([part[rows, :] for part in parts]) * scale
        g[:, b * TILE : (b + 1) * TILE] = value.astype(g.dtype)


def total(parts, scale, own, width):
    outs = [jax.ShapeDtypeStruct((a * RING, TILE), jnp.float32) for a in A_ROWS]
    outs.append(jax.ShapeDtypeStruct((own, width // 2), jnp.bfloat16))
    kernel = functools.partial(total_kernel, scale)
    return call(kernel, "total", outs, [VMEM] * RING)(*parts)


def place_kernel(ats, where, *refs):
    for h, at in enumerate(ats):
        out = refs[len(ats) * RING + h]
        for shift in range(RING):
            piece = refs[h * RING + shift]
            rows = piece.shape[0]
            to = pl.multiple_of(plus(where[at], -shift) * rows, 8)
            out[pl.ds(to, rows), :] = piece[...]


def place(where, halves, ats):
    flat = [a for half in halves for a in half]
    outs = [jax.ShapeDtypeStruct((half[0].shape[0] * RING, TILE), jnp.float32) for half in halves]
    kernel = functools.partial(place_kernel, ats)
    return call(kernel, "place", outs, [SMEM] + [VMEM] * len(flat))(where, *flat)


def send(a, axis, shift):
    return lax.ppermute(a, axis, [(i, (i + shift) % RING) for i in range(RING)])


def swap(half, axis):
    return [half[0]] + [send(half[s], axis, s) for s in range(1, RING)]


def spread(a, axis):
    return [a] + [send(a, axis, s) for s in range(1, RING)]


def row_of(x, t):
    return jnp.broadcast_to(x[t : t + 1, :], x.shape)


def column_of(x, t):
    return jnp.broadcast_to(x[:, t : t + 1], x.shape)


def inverse_of(x):
    guess = pltpu.reciprocal(x, approx=True)
    return guess * (2.0 - x * guess)


def invert_tile(tile):
    lane = lax.broadcasted_iota(jnp.int32, (8, TILE), 1)
    sub = lax.broadcasted_iota(jnp.int32, (8, TILE), 0)
    rows = tile[0:8, :]
    columns = [column_of(rows, t) for t in range(8)]
    for start in range(0, TILE, 8):
        inside = (lane >= start) & (lane < start + 8)
        strip = jnp.where(inside, (lane - start == sub).astype(jnp.float32), rows)
        scale = strip
        for t in range(8):
            here = sub == t
            pivot = inverse_of(row_of(columns[t], t))
            scale = jnp.where(here, pivot, scale)
            ratio = jnp.where(here, 0.0, columns[t]) * pivot
            for j in range(t + 1, 8):
                columns[j] = columns[j] - ratio * row_of(columns[j], t)
            strip = strip - ratio * row_of(strip, t)
        strip = strip * scale
        pivots = [row_of(strip, t) for t in range(8)]
        later = list(range(start + 8, TILE, 8)) + list(range(0, start, 8))
        for other in later:
            block = tile[other : other + 8, :]
            left = jnp.where(inside, 0.0, block)
            for t in range(8):
                left = left - column_of(block, start + t) * pivots[t]
            tile[other : other + 8, :] = left
            if other == start + 8:
                rows = left
                columns = [column_of(rows, other + t) for t in range(8)]
        tile[start : start + 8, :] = strip


def dot(a, b, contract=(1, 0)):
    return lax.dot_general(
        a,
        b,
        (((contract[0],), (contract[1],)), ((), ())),
        preferred_element_type=jnp.float32,
        precision=lax.Precision.HIGHEST,
    )


def at_tile(k):
    return pl.ds(pl.multiple_of(k * TILE, TILE), TILE)


def eliminate(w, y, tile):
    tiles = w.shape[0] // TILE

    def step(k, carry):
        here = at_tile(k)
        tile[...] = w[here, here]
        invert_tile(tile)
        w[here, here] = tile[...]
        for k0 in range(0, tiles - 1, 2):

            @pl.when((k == k0) | ((k == k0 + 1) & (k0 + 2 < tiles)))
            def _():
                second = k != k0
                lo = (k0 + 1) * TILE
                first = jnp.where(second, 0.0, w[here, lo : lo + TILE])
                scaled = dot(tile[...], first)
                w[here, lo : lo + TILE] = jnp.where(second, tile[...], scaled)
                panel = first
                if k0 + 2 < tiles:
                    rest = w[here, lo + TILE :]
                    more = dot(tile[...], rest)
                    w[here, lo + TILE :] = more
                    panel = jnp.concatenate([first, rest], axis=1)
                    scaled = jnp.concatenate([scaled, more], axis=1)
                y[:, lo:] -= dot(y[:, here], scaled)
                turned = panel.T
                for i in range(k0 + 1, tiles):
                    o = (i - k0 - 1) * TILE
                    w[i * TILE : (i + 1) * TILE, i * TILE :] -= dot(
                        turned[o : o + TILE, :], scaled[:, o:]
                    )

        return carry

    lax.fori_loop(0, tiles, step, 0)


def substitute_forward(w, y):
    half = w.shape[0] // TILE // 2
    for group in range(2):
        lo = group * half * TILE

        def step(k, carry):
            here = at_tile(k)
            known = y[:, here]
            y[:, lo:] -= dot(known, w[here, lo:])
            y[:, here] = known
            return carry

        lax.fori_loop(group * half, (group + 1) * half, step, 0)


def substitute_back(w, y, x):
    half = w.shape[0] // TILE // 2
    x[...] = jnp.zeros_like(x)
    for group in (1, 0):
        lo = group * half * TILE

        def step(n, carry):
            here = at_tile((group + 1) * half - 1 - n)
            x[:, here] = dot(y[:, here], w[here, here]) - dot(x[:, lo:], w[here, lo:], (1, 1))
            return carry

        lax.fori_loop(0, half, step, 0)


def fill(where, shift, table, pieces, w):
    line = lax.broadcasted_iota(jnp.int32, (TILE, TILE), 0)
    damp = jnp.where(line == lax.broadcasted_iota(jnp.int32, (TILE, TILE), 1), shift[0], 0.0)
    base = 0
    for h, at in enumerate((AT_X, AT_Y)):
        count = pieces[h * RING].shape[0] // TILE
        for s in range(RING):
            for b in range(count):
                n = base + plus(where[at], -s) * count + b
                i, j = table[0, n], table[1, n]
                block = pieces[h * RING + s][b * TILE : (b + 1) * TILE, :]
                block = block + jnp.where(i == j, 1.0, 0.0) * damp
                rows = pl.ds(pl.multiple_of(i * TILE, TILE), TILE)
                w[rows, pl.ds(pl.multiple_of(j * TILE, TILE), TILE)] = block
        base += count * RING
    tiles = w.shape[0] // TILE
    for i in range(tiles):
        for j in range(i // (tiles // 2) * (tiles // 2), i):
            w[i * TILE : (i + 1) * TILE, j * TILE : (j + 1) * TILE] = jnp.zeros_like(damp)


def times_kept(kept, held, y, x):
    pltpu.sync_copy(kept, held)
    high = y[...].astype(jnp.bfloat16)
    rest = (y[...] - high.astype(jnp.float32)).astype(jnp.bfloat16)
    low = (y[...] - high.astype(jnp.float32) - rest.astype(jnp.float32)).astype(jnp.bfloat16)
    left = jnp.concatenate([high, rest, low], axis=0)
    out = jnp.dot(left, held[...], preferred_element_type=jnp.float32)
    n = y.shape[0]
    x[...] = out[:n] + (out[n : 2 * n] + out[2 * n :])


def left_kernel(where, refresh, shift, table, low, high, kept, *refs):
    pieces, (w, x, y, tile, held) = refs[: 2 * RING], refs[2 * RING :]
    half = low.shape[1]
    y[:, :half] = low[...].astype(y.dtype)
    y[:, half:] = high[...].astype(y.dtype)
    fresh = refresh[0] != 0

    @pl.when(fresh)
    def _():
        fill(where, shift, table, pieces, w)
        eliminate(w, y, tile)
        substitute_back(w, y, x)

    @pl.when(jnp.logical_not(fresh))
    def _():
        times_kept(kept, held, y, x)


def left_solve(where, refresh, shift, pieces, low, high, kept):
    rows, width = low.shape[0], kept.shape[0]
    table = jnp.asarray(np.array(upper(width // TILE), np.int32).T)
    outs = [
        jax.ShapeDtypeStruct((width, width), jnp.float32),
        jax.ShapeDtypeStruct((rows, width), jnp.float32),
    ]
    return call(
        left_kernel,
        "left_solve",
        outs,
        [SMEM, SMEM, SMEM, SMEM, VMEM, VMEM, pl.BlockSpec(memory_space=pl.ANY)]
        + [VMEM] * len(pieces),
        [
            pltpu.VMEM((rows, width), jnp.float32),
            pltpu.VMEM((TILE, TILE), jnp.float32),
            pltpu.VMEM(kept.shape, kept.dtype),
        ],
        3_000_000_000,
        mib=12,
    )(where, refresh, shift, table, low, high, kept, *pieces)


def right_kernel(refresh, step, w, b, kept, out, y, x, held):
    fresh = refresh[0] != 0
    y[...] = b[...]

    @pl.when(fresh)
    def _():
        substitute_forward(w, y)
        substitute_back(w, y, x)

    @pl.when(jnp.logical_not(fresh))
    def _():
        times_kept(kept, held, y, x)

    out[...] = (x[...] * step[0]).astype(out.dtype)


def right_solve(refresh, step, w, b, kept):
    return call(
        right_kernel,
        "right_solve",
        jax.ShapeDtypeStruct(b.shape, jnp.bfloat16),
        [SMEM, SMEM, VMEM, VMEM, pl.BlockSpec(memory_space=pl.ANY)],
        [
            pltpu.VMEM(b.shape, jnp.float32),
            pltpu.VMEM(b.shape, jnp.float32),
            pltpu.VMEM(kept.shape, kept.dtype),
        ],
        mib=12,
    )(refresh, step, w, b, kept)


def body(layer_inputs, out_grads, damping, owners, old_inverse, step_size):
    y, z, x = lax.axis_index("y"), lax.axis_index("zh"), lax.axis_index("x")
    layer, side = lax.axis_index("zl"), lax.axis_index("core")
    parts = RING**3
    width = layer_inputs.shape[2]
    own = width // parts
    scale = 1.0 / (layer_inputs.shape[1] * parts)
    factor_id = 2 * layer + side
    fresh = (owners[factor_id] < parts).astype(jnp.int32)[None]
    where = jnp.stack([x, y, z, layer, side]).astype(jnp.int32)
    shift = damping[factor_id][None]
    step = step_size[layer][None]
    kept = old_inverse[0]

    pieces = local_stats(where, layer_inputs, out_grads)
    a0, a1 = split_sum(where, (swap(pieces[:RING], "x"), swap(pieces[RING:], "y")), (AT_Y, AT_X))
    both = join_sum(where, (swap(a0, "y"), swap(a1, "x")))
    a0, a1, high = total(swap(both, "zh"), scale, own, width)
    a0, a1 = place(where, (spread(a0, "y"), spread(a1, "x")), (AT_Y, AT_X))
    a0, a1 = spread(a0, "x"), spread(a1, "y")
    low = lax.ppermute(high, "core", [(0, 1)])

    w, v = left_solve(where, fresh, shift, a0 + a1, low, high, kept)
    v = v.reshape(own, parts, own).transpose(1, 0, 2).reshape(parts, own * own // TILE, TILE)
    v = lax.ppermute(v, "core", [(1, 0)])
    v = lax.all_to_all(v, ("y", "zh", "x"), split_axis=0, concat_axis=0)
    v = v.reshape(parts * own, own).T
    mine = right_solve(fresh, step, w, v, kept)
    every = lax.all_gather(mine, ("zl", "core"), axis=0)
    return every[0::2]


def solution(mesh):
    split = Mesh(mesh.devices.reshape(RING, RING, RING, 2, 2), ("y", "zh", "x", "zl", "core"))
    tokens = P(None, ("y", "zh", "x"), None)
    placed = (tokens, tokens, P(), P(), P(("zl", "core"), None, None), P())
    return jax.shard_map(
        body, mesh=split, in_specs=placed, out_specs=tokens, check_vma=False
    )
```

```python
import functools

import jax
import jax.numpy as jnp
import numpy as np
from jax import lax
from jax.experimental import pallas as pl
from jax.experimental.pallas import tpu as pltpu
from jax.sharding import Mesh
from jax.sharding import PartitionSpec as P


RING = 4
TILE = 128
VMEM = pl.BlockSpec(memory_space=pltpu.VMEM)
SMEM = pl.BlockSpec(memory_space=pltpu.SMEM)
AT_X, AT_Y, AT_Z, AT_LAYER, AT_SIDE = range(5)


def params(mib):
    return pltpu.CompilerParams(vmem_limit_bytes=mib << 20)


def call(kernel, name, out_shape, in_specs, scratch=(), flops=0, aliases=None, mib=4):
    return pl.pallas_call(
        kernel,
        out_shape=out_shape,
        in_specs=in_specs,
        out_specs=jax.tree.map(lambda _: VMEM, out_shape),
        scratch_shapes=scratch,
        compiler_params=params(mib),
        cost_estimate=pl.CostEstimate(flops=flops, transcendentals=0, bytes_accessed=0),
        input_output_aliases=aliases or {},
        name=name,
    )


def upper(tiles):
    return [(i, j) for i in range(tiles) for j in range(i, tiles)]


def plus(coordinate, shift):
    return lax.rem(coordinate + shift + RING, RING)


A_ROWS = (40, 32)
GRAD_ROWS = 32
CHUNK = tuple(a + GRAD_ROWS for a in A_ROWS)


def stats_kernel(where, inputs, grads, *refs):
    outs, (source, factor, slab) = refs[:-3], refs[-3:]
    width = inputs.shape[1]
    tiles = width // TILE
    side = where[AT_SIDE]

    @pl.when(side == 0)
    def _():
        source[...] = inputs[...]

    @pl.when(side != 0)
    def _():
        source[...] = grads[...]

    contract = (((0,), (0,)), ((), ()))
    n = 0
    for i in range(tiles):
        rows = lax.dot_general(
            source[:, i * TILE : (i + 1) * TILE],
            source[:, i * TILE :],
            contract,
            preferred_element_type=jnp.float32,
        )
        for j in range(tiles - i):
            factor[n * TILE : (n + 1) * TILE, :] = rows[:, j * TILE : (j + 1) * TILE]
            n += 1
    half = width // 2
    mine = grads[:, pl.ds(pl.multiple_of(side * half, half), half)]
    slab[...] = lax.dot_general(inputs[...], mine, contract, preferred_element_type=jnp.float32)
    own = width // RING**3
    for h, at in enumerate((AT_X, AT_Y)):
        base = 0 if h == 0 else A_ROWS[0] * RING**3
        to_x, to_y = (1, 16) if h == 0 else (16, 1)
        for shift in range(RING):
            out = outs[h * RING + shift]
            chunk = plus(where[at], shift)
            for second in range(RING):
                for z in range(RING):
                    piece = second * RING + z
                    o = piece * CHUNK[h]
                    at_a = base + (chunk * RING * RING + piece) * A_ROWS[h]
                    out[o : o + A_ROWS[h], :] = factor[
                        pl.ds(pl.multiple_of(at_a, 8), A_ROWS[h]), :
                    ]
                    device = chunk * to_x + second * to_y + z * RING
                    at_g = pl.ds(pl.multiple_of(device * own, 16), own)
                    for b in range(GRAD_ROWS // own):
                        lanes = (h * (GRAD_ROWS // own) + b) * TILE
                        to = o + A_ROWS[h] + b * own
                        out[to : to + own, :] = slab[at_g, lanes : lanes + TILE]


def local_stats(where, inputs, grads):
    tokens, width = inputs.shape
    tiles = width // TILE
    outs = [
        jax.ShapeDtypeStruct((c * RING * RING, TILE), jnp.float32)
        for c in CHUNK
        for _ in range(RING)
    ]
    return call(
        stats_kernel,
        "local_stats",
        outs,
        [SMEM, VMEM, VMEM],
        [
            pltpu.VMEM((tokens, width), inputs.dtype),
            pltpu.VMEM((len(upper(tiles)) * TILE, TILE), jnp.float32),
            pltpu.VMEM((width, width // 2), jnp.float32),
        ],
        mib=12,
    )(where, inputs, grads)


def four(parts):
    return (parts[0] + parts[1]) + (parts[2] + parts[3])


def split_kernel(ats, where, *refs):
    for h, at in enumerate(ats):
        ins = refs[h * RING : (h + 1) * RING]
        outs = refs[(len(ats) + h) * RING : (len(ats) + h + 1) * RING]
        rows = outs[0].shape[0]
        for shift in range(RING):
            part = pl.ds(pl.multiple_of(plus(where[at], shift) * rows, 8), rows)
            outs[shift][...] = four([ref[part, :] for ref in ins])


def split_sum(where, halves, ats):
    flat = [a for half in halves for a in half]
    outs = [jax.ShapeDtypeStruct((a.shape[0] // RING, TILE), a.dtype) for a in flat]
    kernel = functools.partial(split_kernel, ats)
    got = call(kernel, "split_sum", outs, [SMEM] + [VMEM] * len(flat))(where, *flat)
    return got[:RING], got[RING:]


def join_kernel(where, *refs):
    outs = refs[2 * RING :]
    at = 0
    for h, rows in enumerate(CHUNK):
        ins = refs[h * RING : (h + 1) * RING]
        for z in range(RING):
            o = z * rows
            part = four([ref[o : o + A_ROWS[h], :] for ref in ins])
            for out in outs:
                out[at : at + A_ROWS[h], :] = part
            at += A_ROWS[h]
    for h, rows in enumerate(CHUNK):
        ins = refs[h * RING : (h + 1) * RING]
        for shift, out in enumerate(outs):
            o = pl.multiple_of(plus(where[AT_Z], shift) * rows + A_ROWS[h], 8)
            out[at : at + GRAD_ROWS, :] = four([ref[pl.ds(o, GRAD_ROWS), :] for ref in ins])
        at += GRAD_ROWS


def join_sum(where, halves):
    flat = [a for half in halves for a in half]
    rows = RING * sum(A_ROWS) + 2 * GRAD_ROWS
    outs = [jax.ShapeDtypeStruct((rows, TILE), jnp.float32)] * RING
    return call(join_kernel, "join_sum", outs, [SMEM] + [VMEM] * len(flat))(where, *flat)


def total_kernel(scale, *refs):
    parts, (a0, a1, g) = refs[:RING], refs[RING:]
    o = 0
    own = g.shape[0]
    for a in (a0, a1):
        rows = slice(o, o + a.shape[0])
        a[...] = four([part[rows, :] for part in parts]) * scale
        o += a.shape[0]
    for b in range(2 * GRAD_ROWS // own):
        rows = slice(o + b * own, o + (b + 1) * own)
        value = four([part[rows, :] for part in parts]) * scale
        g[:, b * TILE : (b + 1) * TILE] = value.astype(g.dtype)


def total(parts, scale, own, width):
    outs = [jax.ShapeDtypeStruct((a * RING, TILE), jnp.float32) for a in A_ROWS]
    outs.append(jax.ShapeDtypeStruct((own, width // 2), jnp.bfloat16))
    kernel = functools.partial(total_kernel, scale)
    return call(kernel, "total", outs, [VMEM] * RING)(*parts)


def place_kernel(ats, where, *refs):
    for h, at in enumerate(ats):
        out = refs[len(ats) * RING + h]
        for shift in range(RING):
            piece = refs[h * RING + shift]
            rows = piece.shape[0]
            to = pl.multiple_of(plus(where[at], -shift) * rows, 8)
            out[pl.ds(to, rows), :] = piece[...]


def place(where, halves, ats):
    flat = [a for half in halves for a in half]
    outs = [jax.ShapeDtypeStruct((half[0].shape[0] * RING, TILE), jnp.float32) for half in halves]
    kernel = functools.partial(place_kernel, ats)
    return call(kernel, "place", outs, [SMEM] + [VMEM] * len(flat))(where, *flat)


def send(a, axis, shift):
    return lax.ppermute(a, axis, [(i, (i + shift) % RING) for i in range(RING)])


def swap(half, axis):
    return [half[0]] + [send(half[s], axis, s) for s in range(1, RING)]


def spread(a, axis):
    return [a] + [send(a, axis, s) for s in range(1, RING)]


def row_of(x, t):
    return jnp.broadcast_to(x[t : t + 1, :], x.shape)


def column_of(x, t):
    return jnp.broadcast_to(x[:, t : t + 1], x.shape)


def inverse_of(x):
    guess = pltpu.reciprocal(x, approx=True)
    return guess * (2.0 - x * guess)


def invert_tile(tile):
    lane = lax.broadcasted_iota(jnp.int32, (8, TILE), 1)
    sub = lax.broadcasted_iota(jnp.int32, (8, TILE), 0)
    rows = tile[0:8, :]
    columns = [column_of(rows, t) for t in range(8)]
    for start in range(0, TILE, 8):
        inside = (lane >= start) & (lane < start + 8)
        strip = jnp.where(inside, (lane - start == sub).astype(jnp.float32), rows)
        scale = strip
        for t in range(8):
            here = sub == t
            pivot = inverse_of(row_of(columns[t], t))
            scale = jnp.where(here, pivot, scale)
            ratio = jnp.where(here, 0.0, columns[t]) * pivot
            for j in range(t + 1, 8):
                columns[j] = columns[j] - ratio * row_of(columns[j], t)
            strip = strip - ratio * row_of(strip, t)
        strip = strip * scale
        pivots = [row_of(strip, t) for t in range(8)]
        later = list(range(start + 8, TILE, 8)) + list(range(0, start, 8))
        for other in later:
            block = tile[other : other + 8, :]
            left = jnp.where(inside, 0.0, block)
            for t in range(8):
                left = left - column_of(block, start + t) * pivots[t]
            tile[other : other + 8, :] = left
            if other == start + 8:
                rows = left
                columns = [column_of(rows, other + t) for t in range(8)]
        tile[start : start + 8, :] = strip


def dot(a, b, contract=(1, 0)):
    return lax.dot_general(
        a,
        b,
        (((contract[0],), (contract[1],)), ((), ())),
        preferred_element_type=jnp.float32,
        precision=lax.Precision.HIGHEST,
    )


def at_tile(k):
    return pl.ds(pl.multiple_of(k * TILE, TILE), TILE)


def eliminate(w, y, tile):
    tiles = w.shape[0] // TILE

    def step(k, carry):
        here = at_tile(k)
        tile[...] = w[here, here]
        invert_tile(tile)
        w[here, here] = tile[...]
        for k0 in range(0, tiles - 1, 2):

            @pl.when((k == k0) | ((k == k0 + 1) & (k0 + 2 < tiles)))
            def _():
                second = k != k0
                lo = (k0 + 1) * TILE
                first = jnp.where(second, 0.0, w[here, lo : lo + TILE])
                scaled = dot(tile[...], first)
                w[here, lo : lo + TILE] = jnp.where(second, tile[...], scaled)
                panel = first
                if k0 + 2 < tiles:
                    rest = w[here, lo + TILE :]
                    more = dot(tile[...], rest)
                    w[here, lo + TILE :] = more
                    panel = jnp.concatenate([first, rest], axis=1)
                    scaled = jnp.concatenate([scaled, more], axis=1)
                y[:, lo:] -= dot(y[:, here], scaled)
                turned = panel.T
                for i in range(k0 + 1, tiles):
                    o = (i - k0 - 1) * TILE
                    w[i * TILE : (i + 1) * TILE, i * TILE :] -= dot(
                        turned[o : o + TILE, :], scaled[:, o:]
                    )

        return carry

    lax.fori_loop(0, tiles, step, 0)


def substitute_forward(w, y):
    half = w.shape[0] // TILE // 2
    for group in range(2):
        lo = group * half * TILE

        def step(k, carry):
            here = at_tile(k)
            known = y[:, here]
            y[:, lo:] -= dot(known, w[here, lo:])
            y[:, here] = known
            return carry

        lax.fori_loop(group * half, (group + 1) * half, step, 0)


def substitute_back(w, y, x):
    half = w.shape[0] // TILE // 2
    x[...] = jnp.zeros_like(x)
    for group in (1, 0):
        lo = group * half * TILE

        def step(n, carry):
            here = at_tile((group + 1) * half - 1 - n)
            x[:, here] = dot(y[:, here], w[here, here]) - dot(x[:, lo:], w[here, lo:], (1, 1))
            return carry

        lax.fori_loop(0, half, step, 0)


def fill(where, shift, table, pieces, w):
    line = lax.broadcasted_iota(jnp.int32, (TILE, TILE), 0)
    damp = jnp.where(line == lax.broadcasted_iota(jnp.int32, (TILE, TILE), 1), shift[0], 0.0)
    base = 0
    for h, at in enumerate((AT_X, AT_Y)):
        count = pieces[h * RING].shape[0] // TILE
        for s in range(RING):
            for b in range(count):
                n = base + plus(where[at], -s) * count + b
                i, j = table[0, n], table[1, n]
                block = pieces[h * RING + s][b * TILE : (b + 1) * TILE, :]
                block = block + jnp.where(i == j, 1.0, 0.0) * damp
                rows = pl.ds(pl.multiple_of(i * TILE, TILE), TILE)
                w[rows, pl.ds(pl.multiple_of(j * TILE, TILE), TILE)] = block
        base += count * RING
    tiles = w.shape[0] // TILE
    for i in range(tiles):
        for j in range(i // (tiles // 2) * (tiles // 2), i):
            w[i * TILE : (i + 1) * TILE, j * TILE : (j + 1) * TILE] = jnp.zeros_like(damp)


def times_kept(kept, held, y, x):
    pltpu.sync_copy(kept, held)
    high = y[...].astype(jnp.bfloat16)
    rest = (y[...] - high.astype(jnp.float32)).astype(jnp.bfloat16)
    low = (y[...] - high.astype(jnp.float32) - rest.astype(jnp.float32)).astype(jnp.bfloat16)
    left = jnp.concatenate([high, rest, low], axis=0)
    out = jnp.dot(left, held[...], preferred_element_type=jnp.float32)
    n = y.shape[0]
    x[...] = out[:n] + (out[n : 2 * n] + out[2 * n :])


def left_kernel(where, refresh, shift, table, low, high, kept, *refs):
    pieces, (w, x, y, tile, held) = refs[: 2 * RING], refs[2 * RING :]
    half = low.shape[1]
    y[:, :half] = low[...].astype(y.dtype)
    y[:, half:] = high[...].astype(y.dtype)
    fresh = refresh[0] != 0

    @pl.when(fresh)
    def _():
        fill(where, shift, table, pieces, w)
        eliminate(w, y, tile)
        substitute_back(w, y, x)

    @pl.when(jnp.logical_not(fresh))
    def _():
        times_kept(kept, held, y, x)


def left_solve(where, refresh, shift, pieces, low, high, kept):
    rows, width = low.shape[0], kept.shape[0]
    table = jnp.asarray(np.array(upper(width // TILE), np.int32).T)
    outs = [
        jax.ShapeDtypeStruct((width, width), jnp.float32),
        jax.ShapeDtypeStruct((rows, width), jnp.float32),
    ]
    return call(
        left_kernel,
        "left_solve",
        outs,
        [SMEM, SMEM, SMEM, SMEM, VMEM, VMEM, pl.BlockSpec(memory_space=pl.ANY)]
        + [VMEM] * len(pieces),
        [
            pltpu.VMEM((rows, width), jnp.float32),
            pltpu.VMEM((TILE, TILE), jnp.float32),
            pltpu.VMEM(kept.shape, kept.dtype),
        ],
        3_000_000_000,
        mib=12,
    )(where, refresh, shift, table, low, high, kept, *pieces)


def right_kernel(refresh, step, w, b, kept, out, y, x, held):
    fresh = refresh[0] != 0
    y[...] = b[...]

    @pl.when(fresh)
    def _():
        substitute_forward(w, y)
        substitute_back(w, y, x)

    @pl.when(jnp.logical_not(fresh))
    def _():
        times_kept(kept, held, y, x)

    out[...] = (x[...] * step[0]).astype(out.dtype)


def right_solve(refresh, step, w, b, kept):
    return call(
        right_kernel,
        "right_solve",
        jax.ShapeDtypeStruct(b.shape, jnp.bfloat16),
        [SMEM, SMEM, VMEM, VMEM, pl.BlockSpec(memory_space=pl.ANY)],
        [
            pltpu.VMEM(b.shape, jnp.float32),
            pltpu.VMEM(b.shape, jnp.float32),
            pltpu.VMEM(kept.shape, kept.dtype),
        ],
        mib=12,
    )(refresh, step, w, b, kept)


def body(layer_inputs, out_grads, damping, owners, old_inverse, step_size):
    y, z, x = lax.axis_index("y"), lax.axis_index("zh"), lax.axis_index("x")
    layer, side = lax.axis_index("zl"), lax.axis_index("core")
    parts = RING**3
    width = layer_inputs.shape[2]
    own = width // parts
    scale = 1.0 / (layer_inputs.shape[1] * parts)
    factor_id = 2 * layer + side
    fresh = (owners[factor_id] < parts).astype(jnp.int32)[None]
    where = jnp.stack([x, y, z, layer, side]).astype(jnp.int32)
    shift = damping[factor_id][None]
    step = step_size[layer][None]
    kept = old_inverse[0]

    inputs, grads = (
        lax.dynamic_index_in_dim(a, layer, 0, keepdims=False) for a in (layer_inputs, out_grads)
    )
    pieces = local_stats(where, inputs, grads)
    a0, a1 = split_sum(where, (swap(pieces[:RING], "x"), swap(pieces[RING:], "y")), (AT_Y, AT_X))
    both = join_sum(where, (swap(a0, "y"), swap(a1, "x")))
    a0, a1, high = total(swap(both, "zh"), scale, own, width)
    a0, a1 = place(where, (spread(a0, "y"), spread(a1, "x")), (AT_Y, AT_X))
    a0, a1 = spread(a0, "x"), spread(a1, "y")
    low = lax.ppermute(high, "core", [(0, 1)])

    w, v = left_solve(where, fresh, shift, a0 + a1, low, high, kept)
    v = v.reshape(own, parts, own).transpose(1, 0, 2).reshape(parts, own * own // TILE, TILE)
    v = lax.ppermute(v, "core", [(1, 0)])
    v = lax.all_to_all(v, ("y", "zh", "x"), split_axis=0, concat_axis=0)
    v = v.reshape(parts * own, own).T
    mine = right_solve(fresh, step, w, v, kept)
    every = lax.all_gather(mine, ("zl", "core"), axis=0)
    return every[0::2]


def solution(mesh):
    split = Mesh(mesh.devices.reshape(RING, RING, RING, 2, 2), ("y", "zh", "x", "zl", "core"))
    tokens = P(None, ("y", "zh", "x"), None)
    placed = (tokens, tokens, P(), P(), P(("zl", "core"), None, None), P())
    return jax.shard_map(
        body, mesh=split, in_specs=placed, out_specs=tokens, check_vma=False
    )
```

```python
import functools

import jax
import jax.numpy as jnp
import numpy as np
from jax import lax
from jax.experimental import pallas as pl
from jax.experimental.pallas import tpu as pltpu
from jax.sharding import Mesh
from jax.sharding import PartitionSpec as P


RING = 4
TILE = 128
VMEM = pl.BlockSpec(memory_space=pltpu.VMEM)
SMEM = pl.BlockSpec(memory_space=pltpu.SMEM)
AT_X, AT_Y, AT_Z, AT_LAYER, AT_SIDE = range(5)


def params(mib):
    return pltpu.CompilerParams(vmem_limit_bytes=mib << 20)


def call(kernel, name, out_shape, in_specs, scratch=(), flops=0, aliases=None, mib=4):
    return pl.pallas_call(
        kernel,
        out_shape=out_shape,
        in_specs=in_specs,
        out_specs=jax.tree.map(lambda _: VMEM, out_shape),
        scratch_shapes=scratch,
        compiler_params=params(mib),
        cost_estimate=pl.CostEstimate(flops=flops, transcendentals=0, bytes_accessed=0),
        input_output_aliases=aliases or {},
        name=name,
    )


def upper(tiles):
    return [(i, j) for i in range(tiles) for j in range(i, tiles)]


def plus(coordinate, shift):
    return lax.rem(coordinate + shift + RING, RING)


A_ROWS = (40, 32)
GRAD_ROWS = 32
CHUNK = tuple(a + GRAD_ROWS for a in A_ROWS)


def stats_kernel(where, inputs, grads, *refs):
    outs, (source, factor, slab) = refs[:-3], refs[-3:]
    width = inputs.shape[1]
    tiles = width // TILE
    side = where[AT_SIDE]

    @pl.when(side == 0)
    def _():
        source[...] = inputs[...]

    @pl.when(side != 0)
    def _():
        source[...] = grads[...]

    contract = (((0,), (0,)), ((), ()))
    n = 0
    for i in range(tiles):
        rows = lax.dot_general(
            source[:, i * TILE : (i + 1) * TILE],
            source[:, i * TILE :],
            contract,
            preferred_element_type=jnp.float32,
        )
        for j in range(tiles - i):
            factor[n * TILE : (n + 1) * TILE, :] = rows[:, j * TILE : (j + 1) * TILE]
            n += 1
    half = width // 2
    mine = grads[:, pl.ds(pl.multiple_of(side * half, half), half)]
    slab[...] = lax.dot_general(inputs[...], mine, contract, preferred_element_type=jnp.float32)
    own = width // RING**3
    for h, at in enumerate((AT_X, AT_Y)):
        base = 0 if h == 0 else A_ROWS[0] * RING**3
        to_x, to_y = (1, 16) if h == 0 else (16, 1)
        for shift in range(RING):
            out = outs[h * RING + shift]
            chunk = plus(where[at], shift)
            for second in range(RING):
                for z in range(RING):
                    piece = second * RING + z
                    o = piece * CHUNK[h]
                    at_a = base + (chunk * RING * RING + piece) * A_ROWS[h]
                    out[o : o + A_ROWS[h], :] = factor[
                        pl.ds(pl.multiple_of(at_a, 8), A_ROWS[h]), :
                    ]
                    device = chunk * to_x + second * to_y + z * RING
                    at_g = pl.ds(pl.multiple_of(device * own, 16), own)
                    for b in range(GRAD_ROWS // own):
                        lanes = (h * (GRAD_ROWS // own) + b) * TILE
                        to = o + A_ROWS[h] + b * own
                        out[to : to + own, :] = slab[at_g, lanes : lanes + TILE]


def local_stats(where, inputs, grads):
    tokens, width = inputs.shape
    tiles = width // TILE
    outs = [
        jax.ShapeDtypeStruct((c * RING * RING, TILE), jnp.float32)
        for c in CHUNK
        for _ in range(RING)
    ]
    return call(
        stats_kernel,
        "local_stats",
        outs,
        [SMEM, VMEM, VMEM],
        [
            pltpu.VMEM((tokens, width), inputs.dtype),
            pltpu.VMEM((len(upper(tiles)) * TILE, TILE), jnp.float32),
            pltpu.VMEM((width, width // 2), jnp.float32),
        ],
        mib=12,
    )(where, inputs, grads)


def four(parts):
    return (parts[0] + parts[1]) + (parts[2] + parts[3])


def split_kernel(ats, where, *refs):
    for h, at in enumerate(ats):
        ins = refs[h * RING : (h + 1) * RING]
        outs = refs[(len(ats) + h) * RING : (len(ats) + h + 1) * RING]
        rows = outs[0].shape[0]
        for shift in range(RING):
            part = pl.ds(pl.multiple_of(plus(where[at], shift) * rows, 8), rows)
            outs[shift][...] = four([ref[part, :] for ref in ins])


def split_sum(where, halves, ats):
    flat = [a for half in halves for a in half]
    outs = [jax.ShapeDtypeStruct((a.shape[0] // RING, TILE), a.dtype) for a in flat]
    kernel = functools.partial(split_kernel, ats)
    got = call(kernel, "split_sum", outs, [SMEM] + [VMEM] * len(flat))(where, *flat)
    return got[:RING], got[RING:]


def join_kernel(where, *refs):
    outs = refs[2 * RING :]
    at = 0
    for h, rows in enumerate(CHUNK):
        ins = refs[h * RING : (h + 1) * RING]
        for z in range(RING):
            o = z * rows
            part = four([ref[o : o + A_ROWS[h], :] for ref in ins])
            for out in outs:
                out[at : at + A_ROWS[h], :] = part
            at += A_ROWS[h]
    for h, rows in enumerate(CHUNK):
        ins = refs[h * RING : (h + 1) * RING]
        for shift, out in enumerate(outs):
            o = pl.multiple_of(plus(where[AT_Z], shift) * rows + A_ROWS[h], 8)
            out[at : at + GRAD_ROWS, :] = four([ref[pl.ds(o, GRAD_ROWS), :] for ref in ins])
        at += GRAD_ROWS


def join_sum(where, halves):
    flat = [a for half in halves for a in half]
    rows = RING * sum(A_ROWS) + 2 * GRAD_ROWS
    outs = [jax.ShapeDtypeStruct((rows, TILE), jnp.float32)] * RING
    return call(join_kernel, "join_sum", outs, [SMEM] + [VMEM] * len(flat))(where, *flat)


def total_kernel(scale, *refs):
    parts, (a0, a1, g) = refs[:RING], refs[RING:]
    o = 0
    own = g.shape[0]
    for a in (a0, a1):
        rows = slice(o, o + a.shape[0])
        a[...] = four([part[rows, :] for part in parts]) * scale
        o += a.shape[0]
    for b in range(2 * GRAD_ROWS // own):
        rows = slice(o + b * own, o + (b + 1) * own)
        value = four([part[rows, :] for part in parts]) * scale
        g[:, b * TILE : (b + 1) * TILE] = value.astype(g.dtype)


def total(parts, scale, own, width):
    outs = [jax.ShapeDtypeStruct((a * RING, TILE), jnp.float32) for a in A_ROWS]
    outs.append(jax.ShapeDtypeStruct((own, width // 2), jnp.bfloat16))
    kernel = functools.partial(total_kernel, scale)
    return call(kernel, "total", outs, [VMEM] * RING)(*parts)


def place_kernel(ats, where, *refs):
    for h, at in enumerate(ats):
        out = refs[len(ats) * RING + h]
        for shift in range(RING):
            piece = refs[h * RING + shift]
            rows = piece.shape[0]
            to = pl.multiple_of(plus(where[at], -shift) * rows, 8)
            out[pl.ds(to, rows), :] = piece[...]


def place(where, halves, ats):
    flat = [a for half in halves for a in half]
    outs = [jax.ShapeDtypeStruct((half[0].shape[0] * RING, TILE), jnp.float32) for half in halves]
    kernel = functools.partial(place_kernel, ats)
    return call(kernel, "place", outs, [SMEM] + [VMEM] * len(flat))(where, *flat)


def send(a, axis, shift):
    return lax.ppermute(a, axis, [(i, (i + shift) % RING) for i in range(RING)])


def swap(half, axis):
    return [half[0]] + [send(half[s], axis, s) for s in range(1, RING)]


def spread(a, axis):
    return [a] + [send(a, axis, s) for s in range(1, RING)]


def row_of(x, t):
    return jnp.broadcast_to(x[t : t + 1, :], x.shape)


def column_of(x, t):
    return jnp.broadcast_to(x[:, t : t + 1], x.shape)


def inverse_of(x):
    guess = pltpu.reciprocal(x, approx=True)
    return guess * (2.0 - x * guess)


def invert_tile(tile):
    lane = lax.broadcasted_iota(jnp.int32, (8, TILE), 1)
    sub = lax.broadcasted_iota(jnp.int32, (8, TILE), 0)
    rows = tile[0:8, :]
    columns = [column_of(rows, t) for t in range(8)]
    for start in range(0, TILE, 8):
        inside = (lane >= start) & (lane < start + 8)
        strip = jnp.where(inside, (lane - start == sub).astype(jnp.float32), rows)
        scale = strip
        for t in range(8):
            here = sub == t
            pivot = inverse_of(row_of(columns[t], t))
            scale = jnp.where(here, pivot, scale)
            ratio = jnp.where(here, 0.0, columns[t]) * pivot
            for j in range(t + 1, 8):
                columns[j] = columns[j] - ratio * row_of(columns[j], t)
            strip = strip - ratio * row_of(strip, t)
        strip = strip * scale
        pivots = [row_of(strip, t) for t in range(8)]
        later = list(range(start + 8, TILE, 8)) + list(range(0, start, 8))
        for other in later:
            block = tile[other : other + 8, :]
            left = jnp.where(inside, 0.0, block)
            for t in range(8):
                left = left - column_of(block, start + t) * pivots[t]
            tile[other : other + 8, :] = left
            if other == start + 8:
                rows = left
                columns = [column_of(rows, other + t) for t in range(8)]
        tile[start : start + 8, :] = strip


def dot(a, b, contract=(1, 0)):
    return lax.dot_general(
        a,
        b,
        (((contract[0],), (contract[1],)), ((), ())),
        preferred_element_type=jnp.float32,
        precision=lax.Precision.HIGHEST,
    )


def at_tile(k):
    return pl.ds(pl.multiple_of(k * TILE, TILE), TILE)


def eliminate(w, y, tile):
    tiles = w.shape[0] // TILE

    def step(k, carry):
        here = at_tile(k)
        tile[...] = w[here, here]
        invert_tile(tile)
        w[here, here] = tile[...]
        for k0 in range(0, tiles - 1, 2):

            @pl.when((k == k0) | ((k == k0 + 1) & (k0 + 2 < tiles)))
            def _():
                second = k != k0
                lo = (k0 + 1) * TILE
                first = jnp.where(second, 0.0, w[here, lo : lo + TILE])
                scaled = dot(tile[...], first)
                w[here, lo : lo + TILE] = jnp.where(second, tile[...], scaled)
                panel = first
                if k0 + 2 < tiles:
                    rest = w[here, lo + TILE :]
                    more = dot(tile[...], rest)
                    w[here, lo + TILE :] = more
                    panel = jnp.concatenate([first, rest], axis=1)
                    scaled = jnp.concatenate([scaled, more], axis=1)
                y[:, lo:] -= dot(y[:, here], scaled)
                turned = panel.T
                for i in range(k0 + 1, tiles):
                    o = (i - k0 - 1) * TILE
                    w[i * TILE : (i + 1) * TILE, i * TILE :] -= dot(
                        turned[o : o + TILE, :], scaled[:, o:]
                    )

        return carry

    lax.fori_loop(0, tiles, step, 0)


def substitute_forward(w, y):
    half = w.shape[0] // TILE // 2
    for group in range(2):
        lo = group * half * TILE

        def step(k, carry):
            here = at_tile(k)
            known = y[:, here]
            y[:, lo:] -= dot(known, w[here, lo:])
            y[:, here] = known
            return carry

        lax.fori_loop(group * half, (group + 1) * half, step, 0)


def substitute_back(w, y, x):
    half = w.shape[0] // TILE // 2
    x[...] = jnp.zeros_like(x)
    for group in (1, 0):
        lo = group * half * TILE

        def step(n, carry):
            here = at_tile((group + 1) * half - 1 - n)
            x[:, here] = dot(y[:, here], w[here, here]) - dot(x[:, lo:], w[here, lo:], (1, 1))
            return carry

        lax.fori_loop(0, half, step, 0)


def fill(where, shift, table, pieces, w):
    line = lax.broadcasted_iota(jnp.int32, (TILE, TILE), 0)
    damp = jnp.where(line == lax.broadcasted_iota(jnp.int32, (TILE, TILE), 1), shift[0], 0.0)
    base = 0
    for h, at in enumerate((AT_X, AT_Y)):
        count = pieces[h * RING].shape[0] // TILE
        for s in range(RING):
            for b in range(count):
                n = base + plus(where[at], -s) * count + b
                i, j = table[0, n], table[1, n]
                block = pieces[h * RING + s][b * TILE : (b + 1) * TILE, :]
                block = block + jnp.where(i == j, 1.0, 0.0) * damp
                rows = pl.ds(pl.multiple_of(i * TILE, TILE), TILE)
                w[rows, pl.ds(pl.multiple_of(j * TILE, TILE), TILE)] = block
        base += count * RING
    tiles = w.shape[0] // TILE
    for i in range(tiles):
        for j in range(i // (tiles // 2) * (tiles // 2), i):
            w[i * TILE : (i + 1) * TILE, j * TILE : (j + 1) * TILE] = jnp.zeros_like(damp)


def times_kept(kept, held, y, x):
    pltpu.sync_copy(kept, held)
    high = y[...].astype(jnp.bfloat16)
    rest = (y[...] - high.astype(jnp.float32)).astype(jnp.bfloat16)
    low = (y[...] - high.astype(jnp.float32) - rest.astype(jnp.float32)).astype(jnp.bfloat16)
    left = jnp.concatenate([high, rest, low], axis=0)
    out = jnp.dot(left, held[...], preferred_element_type=jnp.float32)
    n = y.shape[0]
    x[...] = out[:n] + (out[n : 2 * n] + out[2 * n :])


def left_kernel(where, refresh, shift, table, low, high, kept, *refs):
    pieces, (w, x, y, tile, held) = refs[: 2 * RING], refs[2 * RING :]
    half = low.shape[1]
    y[:, :half] = low[...].astype(y.dtype)
    y[:, half:] = high[...].astype(y.dtype)
    fresh = refresh[0] != 0

    @pl.when(fresh)
    def _():
        fill(where, shift, table, pieces, w)
        eliminate(w, y, tile)
        substitute_back(w, y, x)

    @pl.when(jnp.logical_not(fresh))
    def _():
        times_kept(kept, held, y, x)


def left_solve(where, refresh, shift, pieces, low, high, kept):
    rows, width = low.shape[0], kept.shape[0]
    table = jnp.asarray(np.array(upper(width // TILE), np.int32).T)
    outs = [
        jax.ShapeDtypeStruct((width, width), jnp.float32),
        jax.ShapeDtypeStruct((rows, width), jnp.float32),
    ]
    return call(
        left_kernel,
        "left_solve",
        outs,
        [SMEM, SMEM, SMEM, SMEM, VMEM, VMEM, pl.BlockSpec(memory_space=pl.ANY)]
        + [VMEM] * len(pieces),
        [
            pltpu.VMEM((rows, width), jnp.float32),
            pltpu.VMEM((TILE, TILE), jnp.float32),
            pltpu.VMEM(kept.shape, kept.dtype),
        ],
        3_000_000_000,
        mib=12,
    )(where, refresh, shift, table, low, high, kept, *pieces)


def right_kernel(refresh, step, w, b, kept, out, y, x, held):
    fresh = refresh[0] != 0
    y[...] = b[...]

    @pl.when(fresh)
    def _():
        substitute_forward(w, y)
        substitute_back(w, y, x)

    @pl.when(jnp.logical_not(fresh))
    def _():
        times_kept(kept, held, y, x)

    out[...] = (x[...] * step[0]).astype(out.dtype)


def right_solve(refresh, step, w, b, kept):
    return call(
        right_kernel,
        "right_solve",
        jax.ShapeDtypeStruct(b.shape, jnp.bfloat16),
        [SMEM, SMEM, VMEM, VMEM, pl.BlockSpec(memory_space=pl.ANY)],
        [
            pltpu.VMEM(b.shape, jnp.float32),
            pltpu.VMEM(b.shape, jnp.float32),
            pltpu.VMEM(kept.shape, kept.dtype),
        ],
        mib=12,
    )(refresh, step, w, b, kept)


def body(layer_inputs, out_grads, damping, owners, old_inverse, step_size):
    y, z, x = lax.axis_index("y"), lax.axis_index("zh"), lax.axis_index("x")
    layer, side = lax.axis_index("zl"), lax.axis_index("core")
    parts = RING**3
    width = layer_inputs.shape[2]
    own = width // parts
    scale = 1.0 / (layer_inputs.shape[1] * parts)
    factor_id = 2 * layer + side
    fresh = (owners[factor_id] < parts).astype(jnp.int32)[None]
    where = jnp.stack([x, y, z, layer, side]).astype(jnp.int32)
    shift = damping[factor_id][None]
    step = step_size[layer][None]
    kept = old_inverse[0]

    inputs, grads = (
        lax.dynamic_index_in_dim(a, layer, 0, keepdims=False) for a in (layer_inputs, out_grads)
    )
    pieces = local_stats(where, inputs, grads)
    a0, a1 = split_sum(where, (swap(pieces[:RING], "x"), swap(pieces[RING:], "y")), (AT_Y, AT_X))
    both = join_sum(where, (swap(a0, "y"), swap(a1, "x")))
    a0, a1, high = total(swap(both, "zh"), scale, own, width)
    a0, a1 = place(where, (spread(a0, "y"), spread(a1, "x")), (AT_Y, AT_X))
    a0, a1 = spread(a0, "x"), spread(a1, "y")
    low = lax.ppermute(high, "core", [(0, 1)])

    w, v = left_solve(where, fresh, shift, a0 + a1, low, high, kept)
    v = v.reshape(own, parts, own).transpose(1, 0, 2).reshape(parts, own * own // TILE, TILE)
    v = lax.all_to_all(v, ("y", "zh", "x"), split_axis=0, concat_axis=0)
    v = lax.ppermute(v, "core", [(1, 0)])
    v = v.reshape(parts * own, own).T
    mine = right_solve(fresh, step, w, v, kept)
    every = lax.all_gather(mine, ("zl", "core"), axis=0)
    return every[0::2]


def solution(mesh):
    split = Mesh(mesh.devices.reshape(RING, RING, RING, 2, 2), ("y", "zh", "x", "zl", "core"))
    tokens = P(None, ("y", "zh", "x"), None)
    placed = (tokens, tokens, P(), P(), P(("zl", "core"), None, None), P())
    return jax.shard_map(
        body, mesh=split, in_specs=placed, out_specs=tokens, check_vma=False
    )
```
